512 devices in a mesh: gz: 32 (over y, x), gy: 16 (over z, core).
Axes of the slice: x: 4, y: 8, z: 8, core: 2. Of those that a mesh axis runs over, the one named last changes fastest.
Arguments:
- coarse_density: float32 [96, 96, 96], P(None, 'gy'), may hold values from -4 to 4
- density_in: float32 [192, 36864], P('gz', 'gy'), may hold values from -9 to 9
- history: float32 [8, 192, 36864], P(None, 'gz', 'gy'), may hold values from -12 to 12
- atom_cell: int32 [32, 16, 1], P('gz', 'gy'), may hold values from 0 to 13823
- atom_offset: float32 [3, 32, 16, 1], P(None, 'gz', 'gy'), may hold values from 0 to 1
- atom_charge: float32 [32, 16, 1], P('gz', 'gy'), may hold values from -16 to 16
- atom_width: float32 [32, 16, 1], P('gz', 'gy'), may hold values from 0.25 to 1
Outputs:
- residual: float32 [192, 36864], P('gz', 'gy')
- potential: float32 [192, 36864], P('gz', 'gy')
- intersections: float32 [9], replicated
The draws below stay inside these ranges and needn't reach their ends.
Inputs may be any that keep to these rules, and one draw needn't show every extreme that they name: `atom_cell`: the cell lies inside the block of 6 x 12 x 192 fine cells of the slot's first two indices.
All inputs are finite; a program needn't handle non-finite values.
Results may differ from the reference program's by a relative error of at most 0.0003.
Values sent between devices are 32-bit elements; how exact they have to be, the bound alone decides.
A program may use at most 64 MiB of HBM per device.

```python
import math
import jax
import jax.numpy as jnp
from jax import lax

NC = 96
HIST = 8
ATOM_DEV = 1
RC = 4
NF = 192
FZ = 6
FY = 12
N_GZ = 32
N_GY = 16


def midpoint_drawn(extended, dimension, cells_in):

    def window(offset):
        return lax.slice_in_dim(extended, offset, offset + cells_in, axis=dimension)
    even_cells = window(2)
    odd_cells = (9.0 * (window(2) + window(3)) - window(1) - window(4)) / 16.0
    merged = jnp.stack([even_cells, odd_cells], dimension + 1)
    new_shape = list(even_cells.shape)
    new_shape[dimension] = 2 * cells_in
    return merged.reshape(new_shape)


def periodic_drawn(values, dimension):
    length = values.shape[dimension]
    leading = lax.slice_in_dim(values, length - 2, length, axis=dimension)
    trailing = lax.slice_in_dim(values, 0, 2, axis=dimension)
    return jnp.concatenate([leading, values, trailing], dimension)


def coarse_field(key):
    values = jax.random.truncated_normal(jax.random.fold_in(key, 31), -4.0, 4.0, (NC, NC, NC), jnp.float32)
    return values


def common_field(key):
    base = jax.random.truncated_normal(jax.random.fold_in(key, 11), -6.0, 6.0, (NF, NF, NF), jnp.float32)
    return base


def draw_coarse_density(key, part):
    return coarse_field(key)


def draw_density_in(key, part):
    smooth = coarse_field(key)
    for dimension in (2, 1, 0):
        smooth = midpoint_drawn(periodic_drawn(smooth, dimension), dimension, smooth.shape[dimension])
    return (smooth + 0.05 * common_field(key)).reshape(NF, NF * NF)


def draw_history(key, part):
    base = common_field(key)
    gains = jax.random.uniform(jax.random.fold_in(key, 12), (HIST, 1, 1, 1), jnp.float32, 0.3, 1.2)
    noise = jax.random.truncated_normal(jax.random.fold_in(key, 13), -6.0, 6.0, (HIST, NF, NF, NF), jnp.float32)
    return (gains * base[None] + 0.5 * noise).reshape(HIST, NF, NF * NF)


def place_ends(values, rng, least, high):
    longest = values.shape.index(max(values.shape))
    spots = []
    for shift in (0, 1):
        where = [jax.random.randint(jax.random.fold_in(rng, axis), (), 0, length) for axis, length in enumerate(values.shape)]
        where[longest] = (where[longest] + shift) % values.shape[longest]
        spots.append(tuple(where))
    return values.at[spots[0]].set(least).at[spots[1]].set(high)


def levels(key, extent, split, smallest, high):
    def one(dim, parts):
        heights = jax.random.uniform(jax.random.fold_in(jax.random.fold_in(key, 6), dim), (parts,), jnp.float32, smallest / len(split), high / len(split))
        return jnp.repeat(jnp.exp(heights), extent[dim] // parts).reshape((-1,) + (1,) * (len(extent) - dim - 1))

    factor_of = one(*split[0])
    for cut in split[1:]:
        factor_of = factor_of * one(*cut)
    return factor_of


def bell_draw(own_key, dims, deviation, most, shards=(), held_as=jnp.bfloat16):
    level = levels(own_key, dims, shards, -0.22, 0.18) if shards else 1.0
    entries = jax.random.normal(own_key, dims, jnp.float32) * deviation * level
    return jnp.minimum(jnp.maximum(entries, -most), most).astype(held_as)


def setup_inputs(seed: int = 0) -> dict:
    key_list = jax.random.split(jax.random.key(seed), 8)
    return {
        "coarse_density": draw_coarse_density(jax.random.fold_in(key_list[7], 71), 0),
        "density_in": draw_density_in(jax.random.fold_in(key_list[7], 71), 0),
        "history": draw_history(jax.random.fold_in(key_list[7], 71), 0),
        "atom_cell": place_ends(jax.random.randint(key_list[3], (N_GZ, N_GY, ATOM_DEV), 0, FZ * FY * NF), jax.random.fold_in(key_list[3], 1), 0, (FZ * FY * NF) - 1).astype(jnp.int32),
        "atom_offset": jnp.clip(1.0 * jax.random.uniform(key_list[4], (3, N_GZ, N_GY, ATOM_DEV), jnp.float32) ** levels(key_list[4], (3, N_GZ, N_GY, ATOM_DEV), ((1, 32), (2, 16)), -0.2, 0.2), 0.0, 1.0),
        "atom_charge": bell_draw(key_list[5], (N_GZ, N_GY, ATOM_DEV), 4.0, 16.0, ((0, 32), (1, 16)), jnp.float32),
        "atom_width": jnp.clip(jnp.exp(math.log(1.0) - 1.3862944 * jax.random.uniform(key_list[6], (N_GZ, N_GY, ATOM_DEV), jnp.float32) ** levels(key_list[6], (N_GZ, N_GY, ATOM_DEV), ((0, 32), (1, 16)), -0.2, 0.2)), 0.25, 1.0),
    }


def midpoint(extended, dimension, cells_in):
    def window(offset):
        return lax.slice_in_dim(extended, offset, offset + cells_in, axis=dimension)
    even_cells = window(2)
    odd_cells = (9.0 * (window(2) + window(3)) - window(1) - window(4)) / 16.0
    merged = jnp.stack([even_cells, odd_cells], dimension + 1)
    new_shape = list(even_cells.shape)
    new_shape[dimension] = 2 * cells_in
    return merged.reshape(new_shape)


def periodic(values, dimension):
    length = values.shape[dimension]
    leading = lax.slice_in_dim(values, length - 2, length, axis=dimension)
    trailing = lax.slice_in_dim(values, 0, 2, axis=dimension)
    return jnp.concatenate([leading, values, trailing], dimension)


def signed(counter, length):
    return jnp.where(counter < length // 2, counter, counter - length)


def shape_value(squared, charge, exponent):
    factor = charge * (exponent / jnp.pi) ** 1.5
    return factor * jnp.maximum(jnp.exp(-exponent * squared) - jnp.exp(-exponent * float(RC * RC)), 0.0)


def compensation(atom_cell, atom_offset, atom_charge, atom_width):
    plane_cells = FY * NF
    slab_z = jnp.arange(N_GZ, dtype=jnp.int32)[:, None, None] * FZ
    slab_y = jnp.arange(N_GY, dtype=jnp.int32)[None, :, None] * FY
    cell_z = (slab_z + atom_cell // plane_cells).reshape(-1)
    cell_y = (slab_y + (atom_cell // NF) % FY).reshape(-1)
    cell_x = (atom_cell % NF).reshape(-1)
    shifts = jnp.arange(-RC, RC + 2, dtype=jnp.int32)
    offsets = atom_offset.reshape(3, -1)
    charge = atom_charge.reshape(-1)[:, None, None, None]
    exponent = atom_width.reshape(-1)[:, None, None, None]
    index_z = (cell_z[:, None] + shifts[None, :]) % NF
    index_y = (cell_y[:, None] + shifts[None, :]) % NF
    index_x = (cell_x[:, None] + shifts[None, :]) % NF
    moved = shifts[None, :].astype(jnp.float32)
    dist_z = moved - offsets[0][:, None]
    dist_y = moved - offsets[1][:, None]
    dist_x = moved - offsets[2][:, None]
    squared = dist_z[:, :, None, None] ** 2 + dist_y[:, None, :, None] ** 2 + dist_x[:, None, None, :] ** 2
    values = shape_value(squared, charge, exponent)
    density = jnp.zeros((NF, NF, NF), jnp.float32)
    return density.at[index_z[:, :, None, None], index_y[:, None, :, None], index_x[:, None, None, :]].add(values)


def poisson_weight():
    wave = signed(jnp.arange(NF, dtype=jnp.int32), NF)
    squares = wave[:, None, None] * wave[:, None, None] + wave[None, :, None] * wave[None, :, None] + wave[None, None, :] * wave[None, None, :]
    scaled = (2.0 * jnp.pi / NF) ** 2 * jnp.maximum(squares, 1).astype(jnp.float32)
    return jnp.where(squares > 0, 4.0 * jnp.pi / scaled, 0.0).astype(jnp.float32)


def reference(coarse_density, density_in, history, atom_cell, atom_offset, atom_charge, atom_width):
    density_cube = density_in.reshape(NF, NF, NF)
    history_cube = history.reshape(HIST, NF, NF, NF)
    smooth = coarse_density
    for dimension in (2, 1, 0):
        smooth = midpoint(periodic(smooth, dimension), dimension, smooth.shape[dimension])
    residual = smooth + compensation(atom_cell, atom_offset, atom_charge, atom_width) - density_cube
    spectrum = jnp.fft.fftn(residual)
    potential = jnp.real(jnp.fft.ifftn(spectrum * poisson_weight())).astype(jnp.float32)
    cells_all = float(NF) ** 3
    intersections = jnp.concatenate([jnp.sum(history_cube * potential[None], axis=(1, 2, 3)), jnp.sum(residual * potential)[None]]) / cells_all
    return residual.reshape(NF, NF * NF), potential.reshape(NF, NF * NF), intersections
```

```python
import functools

import jax
import jax.numpy as jnp
import numpy as np
from jax import lax
from jax.experimental import pallas as pl
from jax.experimental.pallas import tpu as pltpu
from jax.sharding import PartitionSpec as P

MESH = pl.DeviceIdType.MESH
NC = 96
NF = 192
HIST = 8
RC = 4
FZ = 6
FY = 12
NZ = 32
NY = 16
KX = NF // NY
KY = NF // NZ
STENCIL = ((-1, -1.0 / 16.0), (0, 9.0 / 16.0), (1, 9.0 / 16.0), (2, -1.0 / 16.0))
F32 = jnp.float32
BF16 = jnp.bfloat16


def two(table):
    high = np.asarray(table, np.float32).astype(jnp.bfloat16)
    low = (table - high.astype(np.float64)).astype(np.float32).astype(jnp.bfloat16)
    return high, low


def hartley():
    n = np.arange(NF)
    angle = 2.0 * np.pi / NF * (n[:, None] * n[None, :] % NF)
    return (np.cos(angle) + np.sin(angle)) / np.sqrt(NF)


def tables():
    h = hartley()
    rep = np.zeros((256, NY, 128))
    for j in range(NY):
        for g in range(9):
            rep[:NF, j, g * KX : (g + 1) * KX] = h[:, j * KX : (j + 1) * KX]
    rep = rep.reshape(256, NY * 128)
    by_y = h.reshape(NZ, KY, NY, FY)
    fy = np.zeros((NZ, 8, 2, NY, 8))
    fy[:, :KY, 0] = by_y[:, :, :, :8]
    fy[:, :KY, 1, :, :4] = by_y[:, :, :, 8:]
    fy[:, :KY, 1, :, 4:] = by_y[:, :, :, 8:]
    fy = fy.reshape(256, 256)
    fz = h.reshape(NF, NZ, FZ).transpose(0, 2, 1).reshape(NF, NF)
    ix = np.zeros((256, NC))
    for i in range(NC):
        ix[2 * i, i] = 1.0
        for offset, value in STENCIL:
            ix[2 * i + 1, (i + offset) % NC] += value
    wy = np.zeros((FY, FY // 2 + 3))
    for i in range(FY // 2):
        wy[2 * i, i + 1] = 1.0
        for offset, value in STENCIL:
            wy[2 * i + 1, i + 1 + offset] += value
    place = [(1, 5)] + [(0, r) for r in range(6)] + [(2, 0), (2, 1)]
    spread_y = np.zeros((72, 3, 6, 8))
    for z in range(FZ):
        for y in range(FY):
            row = 8 * z + y if y < 8 else 48 + 8 * (z % 3) + 4 * (z // 3) + y - 8
            for r, (block, coarse_y) in enumerate(place):
                spread_y[row, block, coarse_y, z] = wy[y, r]
    exact = [t.astype(np.float32).astype(jnp.bfloat16) for t in (ix.T, spread_y.reshape(72, 144))]
    return (*two(rep), *two(fy), *two(fy.T), *two(fz), *two(fz.T), *exact)


def split2(value):
    high = value.astype(BF16)
    return high, (value - high.astype(F32)).astype(BF16)


def split3(value):
    high = value.astype(BF16)
    rest = value - high.astype(F32)
    middle = rest.astype(BF16)
    return high, middle, (rest - middle.astype(F32)).astype(BF16)


def dot(a, b):
    return jnp.dot(a, b, preferred_element_type=F32)


def dot_nt(a, b):
    return lax.dot_general(a, b, (((1,), (1,)), ((), ())), preferred_element_type=F32)


def dot3(a, b, product=dot):
    return product(a[0], b[0]) + product(a[1], b[0]) + product(a[0], b[1])


def spread(t, count):
    return count // 2 + ((t + 1) // 2) * (1 - 2 * (t % 2))


def kernel(
    cell_in, offset_in, charge_in, width_in, coarse_in, density_in, history_in, *refs
):
    tables_in, refs = refs[:12], refs[12:]
    residual_out, potential_out, sums_out = refs[:3]
    (
        cell, offset, charge, width, coarse, density, history,
        rep_h, rep_l, fy_h, fy_l, gy_h, gy_l, fz_h, fz_l, gz_h, gz_l, ix, spread_y,
        planes, atoms, field_0, field_1, out_0, out_1, hist_0, hist_1,
        send1, recv1, send2, recv2, send4, recv4, send5, recv5, send_h, recv_h,
        weight, row_a, row_b,
        load_sem, halo_send, halo_recv, atom_send, atom_recv,
        s1, r1, s2, r2, s4, r4, s5, r5, sh, rh, sa, ra, sb, rb,
    ) = refs[3:]
    gz = lax.axis_index("gz")
    gy = lax.axis_index("gy")

    def zy(dz, dy):
        return ((gz + dz + NZ) % NZ, (gy + dy + NY) % NY)

    barrier = pltpu.get_barrier_semaphore()

    def greet_y(t, _):
        j = (gy + spread(t, NY)) % NY
        pl.semaphore_signal(barrier, inc=1, device_id=(gz, j), device_id_type=MESH)
        return 0

    def greet_z(t, _):
        j = (gz + spread(t, NZ)) % NZ
        pl.semaphore_signal(barrier, inc=1, device_id=(j, gy), device_id_type=MESH)
        return 0

    lax.fori_loop(0, NZ - 1, greet_z, 0)
    lax.fori_loop(0, NY - 1, greet_y, 0)
    for dz in (-1, 1):
        for dy in (-1, 1):
            pl.semaphore_signal(barrier, inc=1, device_id=zy(dz, dy), device_id_type=MESH)

    sources = (
        cell_in, offset_in, charge_in, width_in, coarse_in, density_in, tables_in[11], tables_in[10],
        tables_in[0], tables_in[1], tables_in[2], tables_in[3], history_in,
        *tables_in[4:10],
    )
    targets = (
        cell, offset, charge, width, coarse, density, spread_y, ix,
        rep_h, rep_l, fy_h, fy_l, history, gy_h, gy_l, fz_h, fz_l, gz_h, gz_l,
    )
    loads = {}
    for k, (source, target) in enumerate(zip(sources, targets)):
        loads[k] = pltpu.make_async_copy(source, target, load_sem.at[k])
        loads[k].start()

    row8 = lax.broadcasted_iota(jnp.int32, (8, 128), 0)
    lane8 = lax.broadcasted_iota(jnp.int32, (8, 128), 1)
    group = jnp.zeros_like(lane8)
    for c in range(1, 11):
        group = group + (lane8 >= c * KX).astype(jnp.int32)

    def square(counter):
        wave = jnp.where(counter < NF // 2, counter, counter - NF)
        return wave * wave

    wave_yx = (square(gz * KY + group) + square(gy * KX + lane8 - KX * group))[0:1]
    used = (lane8 < KY * KX)[0:1]
    squares = square(lax.broadcasted_iota(jnp.int32, (NF, 128), 0)) + wave_yx
    scaled = (2.0 * np.pi / NF) ** 2 * jnp.maximum(squares, 1).astype(F32)
    weight[...] = jnp.where((squares > 0) & used, 4.0 * np.pi / scaled, 0.0)

    for k in range(4):
        loads[k].wait()

    def whole_tile(value):
        return jnp.broadcast_to(value, (8, 128))

    site = whole_tile(cell[0].astype(F32))
    site_z = jnp.zeros((8, 128), F32)
    for k in range(1, FZ):
        site_z = site_z + (site >= float(k * FY * NF)).astype(F32)
    site = site - site_z * float(FY * NF)
    site_y = jnp.zeros((8, 128), F32)
    for k in range(1, FY):
        site_y = site_y + (site >= float(k * NF)).astype(F32)
    site_x = site - site_y * float(NF)
    own = whole_tile(width[0])
    offsets = offset[0, 0]
    for k, value in enumerate(
        (site_z, site_y, site_x, *(whole_tile(offsets[:, i : i + 1]) for i in range(3)), whole_tile(charge[0]))
    ):
        own = jnp.where(row8 == k, value, own)
    atoms[4] = own

    plane_of = lax.broadcasted_iota(jnp.int32, (8, NC), 1)
    fine_of = lax.broadcasted_iota(jnp.int32, (8, NC), 0)
    away = plane_of - gz * (FZ // 2) - fine_of // 2
    away = jnp.where(away < 0, away + NC, away)
    odd = jnp.zeros((8, NC), F32)
    for shift, value in STENCIL:
        odd = jnp.where(away == shift % NC, value, odd)
    even = jnp.where(away == 0, 1.0, 0.0)
    along_z = jnp.where(fine_of % 2 == 1, odd, even)
    along_z = jnp.where(fine_of < FZ, along_z, 0.0).astype(BF16)
    loads[4].wait()
    for k in range(6):
        parts = split3(coarse[k])
        planes[k] = dot(along_z, parts[0]) + dot(along_z, parts[1]) + dot(along_z, parts[2])

    pl.semaphore_wait(barrier, NY - 1 + NZ - 1 + 4)

    neighbours = []
    for dz in (-1, 1, 0):
        for dy in (-1, 1, 0):
            if (dz, dy) != (0, 0):
                slot = (1 - dz) * 3 + 1 - dy
                neighbours.append(
                    pltpu.make_async_remote_copy(
                        atoms.at[4], atoms.at[slot], atom_send.at[slot], atom_recv.at[slot],
                        device_id=zy(dz, dy), device_id_type=MESH,
                    )
                )
    own_planes = planes.at[pl.ds(0, 6)]
    halos = [
        pltpu.make_async_remote_copy(
            own_planes, planes.at[pl.ds(6 * k, 6)], halo_send.at[k - 1], halo_recv.at[k - 1],
            device_id=zy(0, dy), device_id_type=MESH,
        )
        for k, dy in ((1, 1), (2, -1))
    ]
    for copy in neighbours:
        copy.start()
    for copy in halos:
        copy.start()

    lane128 = lax.broadcasted_iota(jnp.int32, (FZ, 128), 1)
    loads[5].wait()

    def put(y, low, high):
        if y < 8:
            field_0[pl.ds(y, FZ, stride=8), :] = low
            field_1[pl.ds(y, FZ, stride=8), :] = high
        else:
            for half in range(2):
                rows = pl.ds(40 + y + 4 * half, 3, stride=8)
                field_0[rows, :] = low[3 * half : 3 * half + 3]
                field_1[rows, :] = high[3 * half : 3 * half + 3]

    for pair in range(FY // 2):
        a, b, c = (density[:, 384 * pair + 128 * k : 384 * pair + 128 * k + 128] for k in range(3))
        rolled_b = pltpu.roll(b, 64, 1)
        rolled_c = pltpu.roll(c, 64, 1)
        put(2 * pair, a, b)
        put(2 * pair + 1, jnp.where(lane128 < 64, rolled_b, rolled_c), rolled_c)

    x = lax.broadcasted_iota(jnp.int32, (1, 256), 1).astype(F32)
    y_low = row8.astype(F32)
    y_high = jnp.where(row8 < 4, row8 + 8, row8 + 4).astype(F32)
    z = row8.astype(F32)

    def double(value):
        return jnp.concatenate([value, value], axis=1)

    upper = double(row8) < 4

    def charge_of(k):
        tile = atoms[k]
        dz, dy = k // 3 - 1, k % 3 - 1
        exponent = tile[7:8]
        wide = double(tile)
        from_z = (z - float(FZ * dz) - tile[0:1]) - tile[3:4]
        from_low = (y_low - float(FY * dy) - tile[1:2]) - tile[4:5]
        from_high = (y_high - float(FY * dy) - tile[1:2]) - tile[4:5]
        from_x = x - wide[2:3]
        from_x = jnp.where(from_x >= NF / 2, from_x - NF, from_x)
        from_x = jnp.where(from_x < -NF / 2, from_x + NF, from_x)
        from_x = from_x - wide[5:6]
        exp_z = double(jnp.exp(-exponent * (from_z * from_z)))
        exp_x = jnp.exp(-wide[7:8] * (from_x * from_x))
        low = double(jnp.exp(-exponent * (from_low * from_low))) * exp_x
        high = double(jnp.exp(-exponent * (from_high * from_high))) * exp_x
        floor = jnp.exp(-wide[7:8] * float(RC * RC))
        ratio = wide[7:8] / np.pi
        factor = wide[6:7] * (ratio * jnp.sqrt(ratio))
        powers = [low * exp_z[c : c + 1] for c in range(FZ)]
        powers += [high * jnp.where(upper, exp_z[c : c + 1], exp_z[c + 3 : c + 4]) for c in range(3)]
        return [factor * jnp.maximum(power - floor, 0.0) for power in powers]

    total = charge_of(4)
    for k in range(6, 12):
        loads[k].wait()
    for copy in neighbours:
        copy.wait_recv()
    for k in range(9):
        if k != 4:
            total = [a + b for a, b in zip(total, charge_of(k))]

    for copy in halos:
        copy.wait_recv()
    parts = split3(planes[...].reshape(144, NC))
    table = ix[...]
    along_x = dot(parts[0], table) + dot(parts[1], table) + dot(parts[2], table)
    parts = split3(along_x)
    table = spread_y[...]
    smooth = dot(table, parts[0]) + dot(table, parts[1]) + dot(table, parts[2])

    inside = lax.broadcasted_iota(jnp.int32, (8, 256), 1) < NF
    blocks = []
    for g in range(9):
        rows = slice(8 * g, 8 * g + 8)
        given = jnp.concatenate([field_0[rows, :], field_1[rows, :]], axis=1)
        value = jnp.where(inside, smooth[rows] + total[g] - given, 0.0)
        blocks.append(value)
        field_0[rows, :] = value[:, :128]
        field_1[rows, :] = value[:, 128:]

    group256 = double(group)

    def along_x_forward(values, store):
        halves = split2(values)
        for p in range(NY // 2):
            span = slice(256 * p, 256 * p + 256)
            out = dot3(halves, (rep_h[:, span], rep_l[:, span]))
            chosen = out[0:8]
            for g in range(1, 9):
                chosen = jnp.where(group256 >= g, out[8 * g : 8 * g + 8], chosen)
            store(2 * p, chosen[:, :128])
            store(2 * p + 1, chosen[:, 128:])

    def exchange_y(send, recv, ssem, rsem):
        def body(t, _):
            j = (gy + spread(t, NY)) % NY
            pltpu.make_async_remote_copy(
                send.at[j], recv.at[gy], ssem, rsem, device_id=(gz, j), device_id_type=MESH
            ).start()
            return 0

        lax.fori_loop(0, NY - 1, body, 0)
        recv[gy] = send[gy]
        whole = recv.at[pl.ds(0, NY - 1)]
        return pltpu.make_async_copy(whole, whole, rsem), pltpu.make_async_copy(whole, whole, ssem)

    def exchange_z(send, recv, ssem, rsem):
        mine = pl.ds(pl.multiple_of(gz * 8, 8), KY)

        def body(t, _):
            j = (gz + spread(t, NZ)) % NZ
            pltpu.make_async_remote_copy(
                send.at[pl.ds(pl.multiple_of(j * 8, 8), KY)], recv.at[mine],
                ssem, rsem, device_id=(j, gy), device_id_type=MESH,
            ).start()
            return 0

        lax.fori_loop(0, NZ - 1, body, 0)
        recv[mine, :] = send[mine, :]
        whole = recv.at[pl.ds(0, KY * (NZ - 1))]
        return pltpu.make_async_copy(whole, whole, rsem), pltpu.make_async_copy(whole, whole, ssem)

    def store_residual(j, value):
        send1[j] = value

    along_x_forward(jnp.concatenate(blocks, axis=0), store_residual)
    arrived, sent1 = exchange_y(send1, recv1, s1, r1)

    loads[12].wait()
    lane_h = lax.broadcasted_iota(jnp.int32, (HIST, 128), 1)
    for c in range(FZ):
        for pair in range(FY // 2):
            a, b, d = (history[c, :, 384 * pair + 128 * k : 384 * pair + 128 * k + 128] for k in range(3))
            rolled_b = pltpu.roll(b, 64, 1)
            rolled_d = pltpu.roll(d, 64, 1)
            for y, low, high in (
                (2 * pair, a, jnp.where(lane_h < 64, b, 0.0)),
                (2 * pair + 1, jnp.where(lane_h < 64, rolled_b, rolled_d), jnp.where(lane_h < 64, rolled_d, 0.0)),
            ):
                row = 8 * c + y if y < 8 else 48 + 8 * (c % 3) + 4 * (c // 3) + y - 8
                hist_0[pl.ds(row, HIST, stride=72), :] = low
                hist_1[pl.ds(row, HIST, stride=72), :] = high

    def one_history(i, _):
        rows = pl.ds(pl.multiple_of(i * 72, 8), 72)

        def store(j, value):
            send_h[j, i] = value

        along_x_forward(jnp.concatenate([hist_0[rows, :], hist_1[rows, :]], axis=1), store)
        return 0

    lax.fori_loop(0, HIST, one_history, 0)

    groups128 = jnp.concatenate([group] * NY, axis=0)
    rows128 = jnp.concatenate([row8] * NY, axis=0)
    from_upper = (groups128 < 3) & (rows128 < 4)
    from_lower = (groups128 >= 3) & (groups128 < 6) & (rows128 >= 4)
    arrived.wait()
    packed = recv1[...].reshape(128, 128)
    moved = jnp.where(
        from_upper, pltpu.roll(packed, 128 - 72, 1), jnp.where(from_lower, pltpu.roll(packed, 128 - 36, 1), 0.0)
    )
    send2[...] = dot3((fy_h[...], fy_l[...]), split2(jnp.concatenate([packed, moved], axis=0)))
    arrived, sent2 = exchange_z(send2, recv2, s2, r2)
    arrived_h, sent_h = exchange_y(send_h, recv_h, sh, rh)

    def give(out, first, second):
        for pair in range(FY // 2):
            if pair < 4:
                places = ((0, FZ, 2 * pair),)
            else:
                places = ((0, 3, 40 + 2 * pair), (3, 3, 44 + 2 * pair))
            for top, count, row in places:
                low_lanes = lax.broadcasted_iota(jnp.int32, (count, 128), 1) < 64
                a = first[pl.ds(row, count, stride=8), :]
                b = second[pl.ds(row, count, stride=8), :]
                c = pltpu.roll(first[pl.ds(row + 1, count, stride=8), :], 64, 1)
                d = pltpu.roll(second[pl.ds(row + 1, count, stride=8), :], 64, 1)
                tiles = (a, jnp.where(low_lanes, b, c), jnp.where(low_lanes, c, d))
                for k, tile in enumerate(tiles):
                    out[top : top + count, 384 * pair + 128 * k : 384 * pair + 128 * k + 128] = tile

    give(residual_out, field_0, field_1)
    for k in range(13, 19):
        loads[k].wait()
    arrived.wait()

    group1 = group[0:1]

    def swapped(pieces, position):
        result = None
        for b in range(6):
            shift = (KX * (b - position)) % 128
            moved = pltpu.roll(pieces[b], shift, 1) if shift else pieces[b]
            result = moved if result is None else jnp.where(group1 >= b, moved, result)
        return result

    pieces = [recv2[pl.ds(b, NZ, stride=8), :] for b in range(KY)]
    stacked = jnp.concatenate([swapped(pieces, a) for a in range(FZ)], axis=0)
    spectrum = dot3((fz_h[...], fz_l[...]), split2(stacked)) * weight[...]
    back = dot3((gz_h[...], gz_l[...]), split2(spectrum))
    pieces = [back[NZ * a : NZ * a + NZ] for a in range(FZ)]
    for b in range(KY):
        send4[pl.ds(b, NZ, stride=8), :] = swapped(pieces, b)
    arrived, sent4 = exchange_z(send4, recv4, s4, r4)
    arrived.wait()

    rows256 = jnp.concatenate([rows128, rows128], axis=0)
    out = dot3((gy_h[...], gy_l[...]), split2(jnp.where(rows256 < KY, recv4[0:256, :], 0.0)))
    low, high = out[:128], out[128:]
    packed = jnp.where(
        groups128 < 6, low, jnp.where(rows128 < 4, pltpu.roll(high, 72, 1), pltpu.roll(high, 36, 1))
    )
    for j in range(NY):
        send5[j] = packed[8 * j : 8 * j + 8]
    arrived, sent5 = exchange_y(send5, recv5, s5, r5)

    arrived_h.wait()
    terms = [jnp.zeros((8, 128), F32) for _ in range(HIST + 1)]
    for j in range(NY):
        tile = jnp.where(group < 9, packed[8 * j : 8 * j + 8], 0.0)
        for i in range(HIST):
            terms[i] = terms[i] + recv_h[j, i] * tile
        terms[HIST] = terms[HIST] + recv1[j] * tile
    rows = jnp.concatenate(
        [jnp.sum(t, axis=0, keepdims=True) for t in terms] + [jnp.zeros((7, 128), F32)], axis=0
    ) * (1.0 / float(NF) ** 3)
    column = jnp.sum(rows, axis=1, keepdims=True)
    lane_of = lax.broadcasted_iota(jnp.int32, (16, 128), 1)
    row_of = lax.broadcasted_iota(jnp.int32, (16, 128), 0)
    line = jnp.sum(jnp.where(lane_of == row_of, column, 0.0), axis=0, keepdims=True)

    row_b[gz] = line

    def body_b(t, _):
        j = (gz + spread(t, NZ)) % NZ
        pltpu.make_async_remote_copy(
            row_b.at[gz], row_b.at[gz], sb, rb, device_id=(j, gy), device_id_type=MESH
        ).start()
        return 0

    lax.fori_loop(0, NZ - 1, body_b, 0)
    whole_b = row_b.at[pl.ds(0, NZ - 1)]
    pltpu.make_async_copy(whole_b, whole_b, rb).wait()
    row_a[gy] = jnp.sum(row_b[...], axis=0)

    def body_a(t, _):
        j = (gy + spread(t, NY)) % NY
        pltpu.make_async_remote_copy(
            row_a.at[gy], row_a.at[gy], sa, ra, device_id=(gz, j), device_id_type=MESH
        ).start()
        return 0

    lax.fori_loop(0, NY - 1, body_a, 0)

    arrived.wait()
    potential = jnp.zeros((72, 256), F32)
    for p in range(NY // 2):
        pair = split2(jnp.concatenate([recv5[2 * p], recv5[2 * p + 1]], axis=1))
        masked = [
            jnp.concatenate([jnp.where(group256 == g, part.astype(F32), 0.0) for g in range(9)], axis=0).astype(BF16)
            for part in pair
        ]
        span = slice(256 * p, 256 * p + 256)
        potential = potential + dot3(masked, (rep_h[:, span], rep_l[:, span]), dot_nt)
    out_0[0:72, :] = potential[:, :128]
    out_1[0:72, :] = potential[:, 128:]
    give(potential_out, out_0, out_1)

    whole_a = row_a.at[pl.ds(0, NY - 1)]
    pltpu.make_async_copy(whole_a, whole_a, ra).wait()
    sums_out[...] = jnp.sum(row_a[...], axis=0)

    for copy in neighbours:
        copy.wait_send()
    for copy in halos:
        copy.wait_send()
    for copy in (sent1, sent2, sent_h, sent4, sent5):
        copy.wait()
    pltpu.make_async_copy(whole_a, whole_a, sa).wait()
    pltpu.make_async_copy(whole_b, whole_b, sb).wait()


def solution(mesh):
    constants = tables()

    def local(coarse, density, history, cell, offset, charge, width):
        coarse = jnp.transpose(coarse, (1, 0, 2))
        history = jnp.transpose(history, (1, 0, 2))
        offset = jnp.transpose(offset, (1, 2, 3, 0))
        inputs = (cell, offset, charge, width, coarse, density, history)
        inputs = inputs + tuple(jnp.asarray(c) for c in constants)
        vmem = pl.BlockSpec(memory_space=pltpu.VMEM)
        dma = pltpu.SemaphoreType.DMA
        tile = (NY, 8, 128)
        residual, potential, sums = pl.pallas_call(
            kernel,
            out_shape=(
                jax.ShapeDtypeStruct((FZ, FY * NF), F32),
                jax.ShapeDtypeStruct((FZ, FY * NF), F32),
                jax.ShapeDtypeStruct((1, 128), F32),
            ),
            in_specs=[pl.BlockSpec(memory_space=pl.ANY)] * len(inputs),
            out_specs=(vmem, vmem, vmem),
            scratch_shapes=[
                *(pltpu.VMEM(i.shape, i.dtype) for i in inputs),
                pltpu.VMEM((18, 8, NC), F32),
                pltpu.VMEM((9, 8, 128), F32),
                *[pltpu.VMEM((128, 128), F32)] * 4,
                *[pltpu.VMEM((648, 128), F32)] * 2,
                *[pltpu.VMEM(tile, F32)] * 2,
                pltpu.VMEM((256, 128), F32),
                *[pltpu.VMEM((264, 128), F32)] * 3,
                *[pltpu.VMEM(tile, F32)] * 2,
                *[pltpu.VMEM((NY, HIST, 8, 128), F32)] * 2,
                pltpu.VMEM((NF, 128), F32),
                pltpu.VMEM((NY, 1, 128), F32),
                pltpu.VMEM((NZ, 1, 128), F32),
                dma((19,)), dma((2,)), dma((2,)), dma((9,)), dma((9,)),
                *[dma] * 14,
            ],
            compiler_params=pltpu.CompilerParams(collective_id=0, has_side_effects=True),
        )(*inputs)
        return residual, potential, sums[0, : HIST + 1]

    in_specs = (
        P(None, "gy", None),
        P("gz", "gy"),
        P(None, "gz", "gy"),
        P("gz", "gy", None),
        P(None, "gz", "gy", None),
        P("gz", "gy", None),
        P("gz", "gy", None),
    )
    out_specs = (P("gz", "gy"), P("gz", "gy"), P())
    return jax.shard_map(local, mesh=mesh, in_specs=in_specs, out_specs=out_specs, check_vma=False)
```

```python
import functools

import jax
import jax.numpy as jnp
import numpy as np
from jax import lax
from jax.experimental import pallas as pl
from jax.experimental.pallas import tpu as pltpu
from jax.sharding import PartitionSpec as P

MESH = pl.DeviceIdType.MESH
NC = 96
NF = 192
HIST = 8
RC = 4
FZ = 6
FY = 12
NZ = 32
NY = 16
KX = NF // NY
KY = NF // NZ
STENCIL = ((-1, -1.0 / 16.0), (0, 9.0 / 16.0), (1, 9.0 / 16.0), (2, -1.0 / 16.0))
F32 = jnp.float32
BF16 = jnp.bfloat16


def two(table):
    high = np.asarray(table, np.float32).astype(jnp.bfloat16)
    low = (table - high.astype(np.float64)).astype(np.float32).astype(jnp.bfloat16)
    return high, low


def hartley():
    n = np.arange(NF)
    angle = 2.0 * np.pi / NF * (n[:, None] * n[None, :] % NF)
    return (np.cos(angle) + np.sin(angle)) / np.sqrt(NF)


def tables():
    h = hartley()
    rep = np.zeros((256, NY, 128))
    for j in range(NY):
        for g in range(9):
            rep[:NF, j, g * KX : (g + 1) * KX] = h[:, j * KX : (j + 1) * KX]
    rep = rep.reshape(256, NY * 128)
    by_y = h.reshape(NZ, KY, NY, FY)
    fy = np.zeros((NZ, 8, 2, NY, 8))
    fy[:, :KY, 0] = by_y[:, :, :, :8]
    fy[:, :KY, 1, :, :4] = by_y[:, :, :, 8:]
    fy[:, :KY, 1, :, 4:] = by_y[:, :, :, 8:]
    fy = fy.reshape(256, 256)
    fz = h.reshape(NF, NZ, FZ).transpose(0, 2, 1).reshape(NF, NF)
    ix = np.zeros((256, NC))
    for i in range(NC):
        ix[2 * i, i] = 1.0
        for offset, value in STENCIL:
            ix[2 * i + 1, (i + offset) % NC] += value
    wy = np.zeros((FY, FY // 2 + 3))
    for i in range(FY // 2):
        wy[2 * i, i + 1] = 1.0
        for offset, value in STENCIL:
            wy[2 * i + 1, i + 1 + offset] += value
    place = [(1, 5)] + [(0, r) for r in range(6)] + [(2, 0), (2, 1)]
    spread_y = np.zeros((72, 3, 6, 8))
    for z in range(FZ):
        for y in range(FY):
            row = 8 * z + y if y < 8 else 48 + 8 * (z % 3) + 4 * (z // 3) + y - 8
            for r, (block, coarse_y) in enumerate(place):
                spread_y[row, block, coarse_y, z] = wy[y, r]
    exact = [t.astype(np.float32).astype(jnp.bfloat16) for t in (ix.T, spread_y.reshape(72, 144))]
    return (*two(rep), *two(fy), *two(fy.T), *two(fz), *two(fz.T), *exact)


def split2(value):
    high = value.astype(BF16)
    return high, (value - high.astype(F32)).astype(BF16)


def split3(value):
    high = value.astype(BF16)
    rest = value - high.astype(F32)
    middle = rest.astype(BF16)
    return high, middle, (rest - middle.astype(F32)).astype(BF16)


def dot(a, b):
    return jnp.dot(a, b, preferred_element_type=F32)


def dot_nt(a, b):
    return lax.dot_general(a, b, (((1,), (1,)), ((), ())), preferred_element_type=F32)


def dot3(a, b, product=dot):
    return product(a[0], b[0]) + product(a[1], b[0]) + product(a[0], b[1])


def wrap(index, count):
    return jnp.where(index >= count, index - count, index)


def each_partner(me, count, act):
    act(wrap(me + count // 2, count))

    def body(t, _):
        act(wrap(me + count // 2 - t, count))
        act(wrap(me + count // 2 + t, count))
        return 0

    lax.fori_loop(1, count // 2, body, 0, unroll=True)


def kernel(
    cell_in, offset_in, charge_in, width_in, coarse_in, density_in, history_in, *refs
):
    tables_in, refs = refs[:12], refs[12:]
    residual_out, potential_out, sums_out = refs[:3]
    (
        cell, offset, charge, width, coarse, density, history,
        rep_h, rep_l, fy_h, fy_l, gy_h, gy_l, fz_h, fz_l, gz_h, gz_l, ix, spread_y,
        planes, atoms, field_0, field_1, out_0, out_1, hist_0, hist_1,
        send1, recv1, send2, recv2, send4, recv4, send5, recv5, send_h, recv_h,
        weight, row_a, row_b,
        load_sem, halo_send, halo_recv, atom_send, atom_recv,
        s1, r1, s2, r2, s4, r4, s5, r5, sh, rh, sa, ra, sb, rb, ring_z_ready, ring_y_ready, plane_ready,
    ) = refs[3:]
    gz = lax.axis_index("gz")
    gy = lax.axis_index("gy")

    def zy(dz, dy):
        return (wrap(wrap(gz + dz + NZ, NZ), NZ) if dz else gz, wrap(wrap(gy + dy + NY, NY), NY) if dy else gy)

    barrier = pltpu.get_barrier_semaphore()

    def greet(semaphore, z, y):
        pl.semaphore_signal(semaphore, inc=1, device_id=(z, y), device_id_type=MESH)

    column = lax.rem(gz, 4)
    ring_x = [gz - column + lax.rem(column + k, 4) for k in (2, 1, 3)]
    other_core = gy + 1 - 2 * lax.rem(gy, 2)
    greeted = [zy(dz, dy) for dz in (-1, 1) for dy in (-1, 1)]
    greeted += [zy(dz, 0) for dz in (-8, 8)] + [(j, gy) for j in ring_x]
    greeted += [(gz, wrap(wrap(core + dy + NY, NY), NY)) for dy in (-4, 4, -2, 2) for core in (gy, other_core)]
    greeted += [zy(dz, 0) for dz in (-4, 4, -1, 1)] + [(gz, other_core)]
    for z, y in greeted:
        greet(barrier, z, y)

    sources = (
        cell_in, offset_in, charge_in, width_in, coarse_in, density_in, tables_in[11], tables_in[10],
        tables_in[0], tables_in[1], tables_in[2], tables_in[3], history_in,
        *tables_in[4:10],
    )
    targets = (
        cell, offset, charge, width, coarse, density, spread_y, ix,
        rep_h, rep_l, fy_h, fy_l, history, gy_h, gy_l, fz_h, fz_l, gz_h, gz_l,
    )
    loads = {}
    for k, (source, target) in enumerate(zip(sources, targets)):
        loads[k] = pltpu.make_async_copy(source, target, load_sem.at[k])
        loads[k].start()

    row8 = lax.broadcasted_iota(jnp.int32, (8, 128), 0)
    lane8 = lax.broadcasted_iota(jnp.int32, (8, 128), 1)
    group = jnp.zeros_like(lane8)
    for c in range(1, 11):
        group = group + (lane8 >= c * KX).astype(jnp.int32)

    def square(counter):
        wave = jnp.where(counter < NF // 2, counter, counter - NF)
        return wave * wave

    wave_yx = (square(gz * KY + group) + square(gy * KX + lane8 - KX * group))[0:1]
    used = (lane8 < KY * KX)[0:1]
    squares = square(lax.broadcasted_iota(jnp.int32, (NF, 128), 0)) + wave_yx
    scaled = (2.0 * np.pi / NF) ** 2 * jnp.maximum(squares, 1).astype(F32)
    weight[...] = jnp.where((squares > 0) & used, 4.0 * np.pi / scaled, 0.0)

    for k in range(4):
        loads[k].wait()

    def whole_tile(value):
        return jnp.broadcast_to(value, (8, 128))

    site = whole_tile(cell[0].astype(F32))
    site_z = jnp.zeros((8, 128), F32)
    for k in range(1, FZ):
        site_z = site_z + (site >= float(k * FY * NF)).astype(F32)
    site = site - site_z * float(FY * NF)
    site_y = jnp.zeros((8, 128), F32)
    for k in range(1, FY):
        site_y = site_y + (site >= float(k * NF)).astype(F32)
    site_x = site - site_y * float(NF)
    own = whole_tile(width[0])
    offsets = offset[0, 0]
    for k, value in enumerate(
        (site_z, site_y, site_x, *(whole_tile(offsets[:, i : i + 1]) for i in range(3)), whole_tile(charge[0]))
    ):
        own = jnp.where(row8 == k, value, own)
    atoms[4] = own

    plane_of = lax.broadcasted_iota(jnp.int32, (8, NC), 1)
    fine_of = lax.broadcasted_iota(jnp.int32, (8, NC), 0)
    away = plane_of - gz * (FZ // 2) - fine_of // 2
    away = jnp.where(away < 0, away + NC, away)
    odd = jnp.zeros((8, NC), F32)
    for shift, value in STENCIL:
        odd = jnp.where(away == shift % NC, value, odd)
    even = jnp.where(away == 0, 1.0, 0.0)
    along_z = jnp.where(fine_of % 2 == 1, odd, even)
    along_z = jnp.where(fine_of < FZ, along_z, 0.0).astype(BF16)
    loads[4].wait()
    for k in range(6):
        parts = split3(coarse[k])
        planes[k] = dot(along_z, parts[0]) + dot(along_z, parts[1]) + dot(along_z, parts[2])

    pl.semaphore_wait(barrier, len(greeted))

    neighbours = {}
    for dz in (-1, 1, 0):
        for dy in (-1, 1, 0):
            if (dz, dy) != (0, 0):
                slot = (1 - dz) * 3 + 1 - dy
                neighbours[slot] = pltpu.make_async_remote_copy(
                    atoms.at[4], atoms.at[slot], atom_send.at[slot], atom_recv.at[slot],
                    device_id=zy(dz, dy), device_id_type=MESH,
                )
    own_planes = planes.at[pl.ds(0, 6)]
    halos = [
        pltpu.make_async_remote_copy(
            own_planes, planes.at[pl.ds(6 * k, 6)], halo_send.at[k - 1], halo_recv.at[k - 1],
            device_id=zy(0, dy), device_id_type=MESH,
        )
        for k, dy in ((1, 1), (2, -1))
    ]
    for copy in neighbours.values():
        copy.start()
    for copy in halos:
        copy.start()
    for dy in (-4, 4):
        greet(ring_z_ready, *zy(0, dy))
    for dz in (-8, 8):
        greet(ring_y_ready, *zy(dz, 0))

    lane128 = lax.broadcasted_iota(jnp.int32, (FZ, 128), 1)
    loads[5].wait()

    def put(y, low, high):
        if y < 8:
            field_0[pl.ds(y, FZ, stride=8), :] = low
            field_1[pl.ds(y, FZ, stride=8), :] = high
        else:
            for half in range(2):
                rows = pl.ds(40 + y + 4 * half, 3, stride=8)
                field_0[rows, :] = low[3 * half : 3 * half + 3]
                field_1[rows, :] = high[3 * half : 3 * half + 3]

    for pair in range(FY // 2):
        a, b, c = (density[:, 384 * pair + 128 * k : 384 * pair + 128 * k + 128] for k in range(3))
        rolled_b = pltpu.roll(b, 64, 1)
        rolled_c = pltpu.roll(c, 64, 1)
        put(2 * pair, a, b)
        put(2 * pair + 1, jnp.where(lane128 < 64, rolled_b, rolled_c), rolled_c)

    x = lax.broadcasted_iota(jnp.int32, (1, 256), 1).astype(F32)
    y_low = row8.astype(F32)
    y_high = jnp.where(row8 < 4, row8 + 8, row8 + 4).astype(F32)
    z = row8.astype(F32)

    def double(value):
        return jnp.concatenate([value, value], axis=1)

    upper = double(row8) < 4

    def charge_of(k):
        tile = atoms[k]
        dz, dy = k // 3 - 1, k % 3 - 1
        exponent = tile[7:8]
        wide = double(tile)
        from_z = (z - float(FZ * dz) - tile[0:1]) - tile[3:4]
        from_low = (y_low - float(FY * dy) - tile[1:2]) - tile[4:5]
        from_high = (y_high - float(FY * dy) - tile[1:2]) - tile[4:5]
        from_x = x - wide[2:3]
        from_x = jnp.where(from_x >= NF / 2, from_x - NF, from_x)
        from_x = jnp.where(from_x < -NF / 2, from_x + NF, from_x)
        from_x = from_x - wide[5:6]
        exp_z = double(jnp.exp(-exponent * (from_z * from_z)))
        exp_x = jnp.exp(-wide[7:8] * (from_x * from_x))
        low = double(jnp.exp(-exponent * (from_low * from_low))) * exp_x
        high = double(jnp.exp(-exponent * (from_high * from_high))) * exp_x
        floor = jnp.exp(-wide[7:8] * float(RC * RC))
        ratio = wide[7:8] / np.pi
        factor = wide[6:7] * (ratio * jnp.sqrt(ratio))
        powers = [low * exp_z[c : c + 1] for c in range(FZ)]
        powers += [high * jnp.where(upper, exp_z[c : c + 1], exp_z[c + 3 : c + 4]) for c in range(3)]
        return [factor * jnp.maximum(power - floor, 0.0) for power in powers]

    total = charge_of(4)
    for k in range(6, 12):
        loads[k].wait()

    for copy in halos:
        copy.wait_recv()
    parts = split3(planes[...].reshape(144, NC))
    table = ix[...]
    along_x = dot(parts[0], table) + dot(parts[1], table) + dot(parts[2], table)
    parts = split3(along_x)
    table = spread_y[...]
    smooth = dot(table, parts[0]) + dot(table, parts[1]) + dot(table, parts[2])

    for k in (3, 5, 1, 7, 0, 2, 6, 8):
        neighbours[k].wait_recv()
        total = [a + b for a, b in zip(total, charge_of(k))]

    inside = lax.broadcasted_iota(jnp.int32, (8, 256), 1) < NF
    blocks = []
    for g in range(9):
        rows = slice(8 * g, 8 * g + 8)
        given = jnp.concatenate([field_0[rows, :], field_1[rows, :]], axis=1)
        value = jnp.where(inside, smooth[rows] + total[g] - given, 0.0)
        blocks.append(value)
        field_0[rows, :] = value[:, :128]
        field_1[rows, :] = value[:, 128:]

    group256 = double(group)

    def along_x_forward(values, store):
        halves = split2(values)
        for p in range(NY // 2):
            span = slice(256 * p, 256 * p + 256)
            out = dot3(halves, (rep_h[:, span], rep_l[:, span]))
            chosen = out[0:8]
            for g in range(1, 9):
                chosen = jnp.where(group256 >= g, out[8 * g : 8 * g + 8], chosen)
            store(2 * p, chosen[:, :128])
            store(2 * p + 1, chosen[:, 128:])

    def exchange_y(send, recv, ssem, rsem):
        def act(j):
            pltpu.make_async_remote_copy(
                send.at[j], recv.at[gy], ssem, rsem, device_id=(gz, j), device_id_type=MESH
            ).start()

        each_partner(gy, NY, act)
        recv[gy] = send[gy]
        whole = recv.at[pl.ds(0, NY - 1)]
        return pltpu.make_async_copy(whole, whole, rsem), pltpu.make_async_copy(whole, whole, ssem)

    def exchange_z(send, recv, ssem, rsem):
        mine = pl.ds(pl.multiple_of(gz * 8, 8), KY)

        def act(j):
            pltpu.make_async_remote_copy(
                send.at[pl.ds(pl.multiple_of(j * 8, 8), KY)], recv.at[mine],
                ssem, rsem, device_id=(j, gy), device_id_type=MESH,
            ).start()

        each_partner(gz, NZ, act)
        recv[mine, :] = send[mine, :]
        whole = recv.at[pl.ds(0, KY * (NZ - 1))]
        return pltpu.make_async_copy(whole, whole, rsem), pltpu.make_async_copy(whole, whole, ssem)

    def store_residual(j, value):
        send1[j] = value

    along_x_forward(jnp.concatenate(blocks, axis=0), store_residual)
    pl.semaphore_wait(ring_z_ready, 2)
    arrived, sent1 = exchange_y(send1, recv1, s1, r1)

    pl.semaphore_wait(ring_y_ready, 2)
    for j in ring_x:
        greet(plane_ready, j, gy)

    loads[12].wait()
    lane_h = lax.broadcasted_iota(jnp.int32, (HIST, 128), 1)
    for c in range(FZ):
        for pair in range(FY // 2):
            a, b, d = (history[c, :, 384 * pair + 128 * k : 384 * pair + 128 * k + 128] for k in range(3))
            rolled_b = pltpu.roll(b, 64, 1)
            rolled_d = pltpu.roll(d, 64, 1)
            for y, low, high in (
                (2 * pair, a, jnp.where(lane_h < 64, b, 0.0)),
                (2 * pair + 1, jnp.where(lane_h < 64, rolled_b, rolled_d), jnp.where(lane_h < 64, rolled_d, 0.0)),
            ):
                row = 8 * c + y if y < 8 else 48 + 8 * (c % 3) + 4 * (c // 3) + y - 8
                hist_0[pl.ds(row, HIST, stride=72), :] = low
                hist_1[pl.ds(row, HIST, stride=72), :] = high

    def one_history(i, _):
        rows = pl.ds(pl.multiple_of(i * 72, 8), 72)

        def store(j, value):
            send_h[j, i] = value

        along_x_forward(jnp.concatenate([hist_0[rows, :], hist_1[rows, :]], axis=1), store)
        return 0

    lax.fori_loop(0, HIST, one_history, 0)

    groups128 = jnp.concatenate([group] * NY, axis=0)
    rows128 = jnp.concatenate([row8] * NY, axis=0)
    from_upper = (groups128 < 3) & (rows128 < 4)
    from_lower = (groups128 >= 3) & (groups128 < 6) & (rows128 >= 4)
    arrived.wait()
    packed = recv1[...].reshape(128, 128)
    moved = jnp.where(
        from_upper, pltpu.roll(packed, 128 - 72, 1), jnp.where(from_lower, pltpu.roll(packed, 128 - 36, 1), 0.0)
    )
    send2[...] = dot3((fy_h[...], fy_l[...]), split2(jnp.concatenate([packed, moved], axis=0)))
    pl.semaphore_wait(plane_ready, 3)
    arrived, sent2 = exchange_z(send2, recv2, s2, r2)
    arrived_h, sent_h = exchange_y(send_h, recv_h, sh, rh)

    def give(out, first, second):
        for pair in range(FY // 2):
            if pair < 4:
                places = ((0, FZ, 2 * pair),)
            else:
                places = ((0, 3, 40 + 2 * pair), (3, 3, 44 + 2 * pair))
            for top, count, row in places:
                low_lanes = lax.broadcasted_iota(jnp.int32, (count, 128), 1) < 64
                a = first[pl.ds(row, count, stride=8), :]
                b = second[pl.ds(row, count, stride=8), :]
                c = pltpu.roll(first[pl.ds(row + 1, count, stride=8), :], 64, 1)
                d = pltpu.roll(second[pl.ds(row + 1, count, stride=8), :], 64, 1)
                tiles = (a, jnp.where(low_lanes, b, c), jnp.where(low_lanes, c, d))
                for k, tile in enumerate(tiles):
                    out[top : top + count, 384 * pair + 128 * k : 384 * pair + 128 * k + 128] = tile

    give(residual_out, field_0, field_1)
    for k in range(13, 19):
        loads[k].wait()
    arrived.wait()

    group1 = group[0:1]

    def swapped(pieces, position):
        result = None
        for b in range(6):
            shift = (KX * (b - position)) % 128
            moved = pltpu.roll(pieces[b], shift, 1) if shift else pieces[b]
            result = moved if result is None else jnp.where(group1 >= b, moved, result)
        return result

    pieces = [recv2[pl.ds(b, NZ, stride=8), :] for b in range(KY)]
    stacked = jnp.concatenate([swapped(pieces, a) for a in range(FZ)], axis=0)
    spectrum = dot3((fz_h[...], fz_l[...]), split2(stacked)) * weight[...]
    back = dot3((gz_h[...], gz_l[...]), split2(spectrum))
    pieces = [back[NZ * a : NZ * a + NZ] for a in range(FZ)]
    for b in range(KY):
        send4[pl.ds(b, NZ, stride=8), :] = swapped(pieces, b)
    arrived, sent4 = exchange_z(send4, recv4, s4, r4)
    arrived.wait()

    rows256 = jnp.concatenate([rows128, rows128], axis=0)
    out = dot3((gy_h[...], gy_l[...]), split2(jnp.where(rows256 < KY, recv4[0:256, :], 0.0)))
    low, high = out[:128], out[128:]
    packed = jnp.where(
        groups128 < 6, low, jnp.where(rows128 < 4, pltpu.roll(high, 72, 1), pltpu.roll(high, 36, 1))
    )
    arrived_h.wait()
    terms = [jnp.zeros((8, 128), F32) for _ in range(HIST + 1)]
    for j in range(NY):
        tile = jnp.where(group < 9, packed[8 * j : 8 * j + 8], 0.0)
        for i in range(HIST):
            terms[i] = terms[i] + recv_h[j, i] * tile
        terms[HIST] = terms[HIST] + recv1[j] * tile
    rows = jnp.concatenate(
        [jnp.sum(t, axis=0, keepdims=True) for t in terms] + [jnp.zeros((7, 128), F32)], axis=0
    ) * (1.0 / float(NF) ** 3)
    column = jnp.sum(rows, axis=1, keepdims=True)
    lane_of = lax.broadcasted_iota(jnp.int32, (16, 128), 1)
    row_of = lax.broadcasted_iota(jnp.int32, (16, 128), 0)
    line = jnp.sum(jnp.where(lane_of == row_of, column, 0.0), axis=0, keepdims=True)

    row_b[gz] = line

    def act_b(j):
        pltpu.make_async_remote_copy(
            row_b.at[gz], row_b.at[gz], sb, rb, device_id=(j, gy), device_id_type=MESH
        ).start()

    each_partner(gz, NZ, act_b)
    for j in range(NY):
        send5[j] = packed[8 * j : 8 * j + 8]
    arrived, sent5 = exchange_y(send5, recv5, s5, r5)
    whole_b = row_b.at[pl.ds(0, NZ - 1)]
    pltpu.make_async_copy(whole_b, whole_b, rb).wait()
    row_a[gy] = jnp.sum(row_b[...], axis=0)

    def act_a(j):
        pltpu.make_async_remote_copy(
            row_a.at[gy], row_a.at[gy], sa, ra, device_id=(gz, j), device_id_type=MESH
        ).start()

    each_partner(gy, NY, act_a)

    arrived.wait()
    potential = jnp.zeros((72, 256), F32)
    for p in range(NY // 2):
        pair = split2(jnp.concatenate([recv5[2 * p], recv5[2 * p + 1]], axis=1))
        masked = [
            jnp.concatenate([jnp.where(group256 == g, part.astype(F32), 0.0) for g in range(9)], axis=0).astype(BF16)
            for part in pair
        ]
        span = slice(256 * p, 256 * p + 256)
        potential = potential + dot3(masked, (rep_h[:, span], rep_l[:, span]), dot_nt)
    out_0[0:72, :] = potential[:, :128]
    out_1[0:72, :] = potential[:, 128:]
    give(potential_out, out_0, out_1)

    whole_a = row_a.at[pl.ds(0, NY - 1)]
    pltpu.make_async_copy(whole_a, whole_a, ra).wait()
    sums_out[...] = jnp.sum(row_a[...], axis=0)[0, : HIST + 1]

    for copy in neighbours.values():
        copy.wait_send()
    for copy in halos:
        copy.wait_send()
    for copy in (sent1, sent2, sent_h, sent4, sent5):
        copy.wait()
    pltpu.make_async_copy(whole_a, whole_a, sa).wait()
    pltpu.make_async_copy(whole_b, whole_b, sb).wait()


def write_out(*refs):
    copies = [pltpu.make_async_copy(refs[k], refs[3 + k], refs[6].at[k]) for k in range(3)]
    for copy in copies:
        copy.start()
    for copy in copies:
        copy.wait()


def solution(mesh):
    constants = tables()

    def local(coarse, density, history, cell, offset, charge, width):
        coarse = jnp.transpose(coarse, (1, 0, 2))
        history = jnp.transpose(history, (1, 0, 2))
        offset = jnp.transpose(offset, (1, 2, 3, 0))
        inputs = (cell, offset, charge, width, coarse, density, history)
        inputs = inputs + tuple(jnp.asarray(c) for c in constants)
        vmem = pl.BlockSpec(memory_space=pltpu.VMEM)
        dma = pltpu.SemaphoreType.DMA
        tile = (NY, 8, 128)
        residual, potential, sums = pl.pallas_call(
            kernel,
            out_shape=(
                pltpu.VMEM((FZ, FY * NF), F32),
                pltpu.VMEM((FZ, FY * NF), F32),
                pltpu.VMEM((HIST + 1,), F32),
            ),
            in_specs=[pl.BlockSpec(memory_space=pltpu.HBM)] * len(inputs),
            out_specs=(vmem, vmem, vmem),
            scratch_shapes=[
                *(pltpu.VMEM(i.shape, i.dtype) for i in inputs),
                pltpu.VMEM((18, 8, NC), F32),
                pltpu.VMEM((9, 8, 128), F32),
                *[pltpu.VMEM((128, 128), F32)] * 4,
                *[pltpu.VMEM((648, 128), F32)] * 2,
                *[pltpu.VMEM(tile, F32)] * 2,
                pltpu.VMEM((256, 128), F32),
                *[pltpu.VMEM((264, 128), F32)] * 3,
                *[pltpu.VMEM(tile, F32)] * 2,
                *[pltpu.VMEM((NY, HIST, 8, 128), F32)] * 2,
                pltpu.VMEM((NF, 128), F32),
                pltpu.VMEM((NY, 1, 128), F32),
                pltpu.VMEM((NZ, 1, 128), F32),
                dma((19,)), dma((2,)), dma((2,)), dma((9,)), dma((9,)),
                *[dma] * 14,
                *[pltpu.SemaphoreType.REGULAR] * 3,
            ],
            compiler_params=pltpu.CompilerParams(collective_id=0, has_side_effects=True),
        )(*inputs)
        results = tuple(pltpu.with_memory_space_constraint(r, pltpu.VMEM) for r in (residual, potential, sums))
        hbm = pl.BlockSpec(memory_space=pltpu.HBM)
        return pl.pallas_call(
            write_out,
            out_shape=tuple(jax.ShapeDtypeStruct(r.shape, F32) for r in results),
            in_specs=[vmem] * 3,
            out_specs=(hbm,) * 3,
            scratch_shapes=[dma((3,))],
        )(*results)

    in_specs = (
        P(None, "gy", None),
        P("gz", "gy"),
        P(None, "gz", "gy"),
        P("gz", "gy", None),
        P(None, "gz", "gy", None),
        P("gz", "gy", None),
        P("gz", "gy", None),
    )
    out_specs = (P("gz", "gy"), P("gz", "gy"), P())
    return jax.shard_map(local, mesh=mesh, in_specs=in_specs, out_specs=out_specs, check_vma=False)
```

```python
import functools

import jax
import jax.numpy as jnp
import numpy as np
from jax import lax
from jax.experimental import pallas as pl
from jax.experimental.pallas import tpu as pltpu
from jax.sharding import PartitionSpec as P

MESH = pl.DeviceIdType.MESH
NC = 96
NF = 192
HIST = 8
EARLY = 3
RC = 4
FZ = 6
FY = 12
NZ = 32
NY = 16
KX = NF // NY
KY = NF // NZ
STENCIL = ((-1, -1.0 / 16.0), (0, 9.0 / 16.0), (1, 9.0 / 16.0), (2, -1.0 / 16.0))
F32 = jnp.float32
BF16 = jnp.bfloat16


def two(table):
    high = np.asarray(table, np.float32).astype(jnp.bfloat16)
    low = (table - high.astype(np.float64)).astype(np.float32).astype(jnp.bfloat16)
    return high, low


def hartley():
    n = np.arange(NF)
    angle = 2.0 * np.pi / NF * (n[:, None] * n[None, :] % NF)
    return (np.cos(angle) + np.sin(angle)) / np.sqrt(NF)


def tables():
    h = hartley()
    rep = np.zeros((256, NY, 128))
    for j in range(NY):
        for g in range(9):
            rep[:NF, j, g * KX : (g + 1) * KX] = h[:, j * KX : (j + 1) * KX]
    rep = rep.reshape(256, NY * 128)
    by_y = h.reshape(NZ, KY, NY, FY)
    fy = np.zeros((NZ, 8, 2, NY, 8))
    fy[:, :KY, 0] = by_y[:, :, :, :8]
    fy[:, :KY, 1, :, :4] = by_y[:, :, :, 8:]
    fy[:, :KY, 1, :, 4:] = by_y[:, :, :, 8:]
    fy = fy.reshape(256, 256)
    fz = h.reshape(NF, NZ, FZ).transpose(0, 2, 1).reshape(NF, NF)
    ix = np.zeros((256, NC))
    for i in range(NC):
        ix[2 * i, i] = 1.0
        for offset, value in STENCIL:
            ix[2 * i + 1, (i + offset) % NC] += value
    wy = np.zeros((FY, FY // 2 + 3))
    for i in range(FY // 2):
        wy[2 * i, i + 1] = 1.0
        for offset, value in STENCIL:
            wy[2 * i + 1, i + 1 + offset] += value
    place = [(1, 5)] + [(0, r) for r in range(6)] + [(2, 0), (2, 1)]
    spread_y = np.zeros((72, 3, 6, 8))
    for z in range(FZ):
        for y in range(FY):
            row = 8 * z + y if y < 8 else 48 + 8 * (z % 3) + 4 * (z // 3) + y - 8
            for r, (block, coarse_y) in enumerate(place):
                spread_y[row, block, coarse_y, z] = wy[y, r]
    exact = [t.astype(np.float32).astype(jnp.bfloat16) for t in (ix.T, spread_y.reshape(72, 144))]
    pieces = {"ix": exact[0], "spread_y": exact[1]}
    for name, table in (("fy", fy), ("gy", fy.T), ("fz", fz), ("gz", fz.T)):
        pieces[name + "_h"], pieces[name + "_l"] = two(table)
    by_span = rep.reshape(256, NY // 2, 256).transpose(1, 0, 2).reshape(-1, 256)
    pieces["rep_h"], pieces["rep_l"] = two(by_span)
    place, stack, row = {}, [], 0
    for name, piece in pieces.items():
        rows, columns = piece.shape
        place[name] = (row, rows, columns)
        stack.append(np.pad(piece, ((0, -rows % 16), (0, 256 - columns))))
        row += rows + -rows % 16
    return np.concatenate(stack, axis=0), place


def split2(value):
    high = value.astype(BF16)
    return high, (value - high.astype(F32)).astype(BF16)


def split3(value):
    high = value.astype(BF16)
    rest = value - high.astype(F32)
    middle = rest.astype(BF16)
    return high, middle, (rest - middle.astype(F32)).astype(BF16)


def dot(a, b):
    return jnp.dot(a, b, preferred_element_type=F32)


def dot_nt(a, b):
    return lax.dot_general(a, b, (((1,), (1,)), ((), ())), preferred_element_type=F32)


def dot3(a, b, product=dot):
    return product(a[0], b[0]) + product(a[1], b[0]) + product(a[0], b[1])


def wrap(index, count):
    return jnp.where(index >= count, index - count, index)


def each_partner(me, count, act):
    act(wrap(me + count // 2, count))

    def body(t, _):
        act(wrap(me + count // 2 - t, count))
        act(wrap(me + count // 2 + t, count))
        return 0

    lax.fori_loop(1, count // 2, body, 0, unroll=True)


def kernel(
    place, cell_in, offset_in, charge_in, width_in, coarse_in, density_in, history_in, tables_in, *refs
):
    residual_out, potential_out, sums_out = refs[:3]
    (
        cell, offset, charge, width, coarse, density, history, all_tables,
        planes, atoms, field_0, field_1, out_0, out_1, hist_0, hist_1,
        send1, recv1, send2, recv2, send4, recv4, send5, recv5, send_g, recv_g, send_h, recv_h,
        weight, row_a, row_b,
        load_sem, halo_send, halo_recv, atom_send, atom_recv,
        s1, r1, s2, r2, s4, r4, s5, r5, sg, rg, sh, rh, sa, ra, sb, rb, ring_z_ready, ring_y_ready, plane_ready,
    ) = refs[3:]
    gz = lax.axis_index("gz")
    gy = lax.axis_index("gy")

    def zy(dz, dy):
        return (wrap(wrap(gz + dz + NZ, NZ), NZ) if dz else gz, wrap(wrap(gy + dy + NY, NY), NY) if dy else gy)

    barrier = pltpu.get_barrier_semaphore()

    def greet(semaphore, z, y):
        pl.semaphore_signal(semaphore, inc=1, device_id=(z, y), device_id_type=MESH)

    column = lax.rem(gz, 4)
    ring_x = [gz - column + lax.rem(column + k, 4) for k in (2, 1, 3)]
    other_core = gy + 1 - 2 * lax.rem(gy, 2)
    greeted = [zy(dz, dy) for dz in (-1, 1) for dy in (-1, 1)]
    greeted += [zy(dz, 0) for dz in (-8, 8)] + [(j, gy) for j in ring_x]
    greeted += [(gz, wrap(wrap(core + dy + NY, NY), NY)) for dy in (-4, 4, -2, 2) for core in (gy, other_core)]
    greeted += [zy(dz, 0) for dz in (-4, 4, -1, 1)] + [(gz, other_core)]
    for z, y in greeted:
        greet(barrier, z, y)

    sources = (
        cell_in, offset_in, charge_in, width_in, coarse_in, density_in, tables_in, history_in,
    )
    targets = (cell, offset, charge, width, coarse, density, all_tables, history)
    loads = {}
    for k, (source, target) in enumerate(zip(sources, targets)):
        loads[k] = pltpu.make_async_copy(source, target, load_sem.at[k])
        loads[k].start()

    def table(name):
        row, rows, columns = place[name]
        return all_tables[row : row + rows, :columns]

    def spans(p):
        return tuple(
            all_tables[place[name][0] + 256 * p : place[name][0] + 256 * p + 256, :]
            for name in ("rep_h", "rep_l")
        )

    row8 = lax.broadcasted_iota(jnp.int32, (8, 128), 0)
    lane8 = lax.broadcasted_iota(jnp.int32, (8, 128), 1)
    group = jnp.zeros_like(lane8)
    for c in range(1, 11):
        group = group + (lane8 >= c * KX).astype(jnp.int32)

    def square(counter):
        wave = jnp.where(counter < NF // 2, counter, counter - NF)
        return wave * wave

    wave_yx = (square(gz * KY + group) + square(gy * KX + lane8 - KX * group))[0:1]
    used = (lane8 < KY * KX)[0:1]
    squares = square(lax.broadcasted_iota(jnp.int32, (NF, 128), 0)) + wave_yx
    scaled = (2.0 * np.pi / NF) ** 2 * jnp.maximum(squares, 1).astype(F32)
    weight[...] = jnp.where((squares > 0) & used, 4.0 * np.pi / scaled, 0.0)

    for k in range(4):
        loads[k].wait()

    def whole_tile(value):
        return jnp.broadcast_to(value, (8, 128))

    site = whole_tile(cell[0].astype(F32))
    site_z = jnp.zeros((8, 128), F32)
    for k in range(1, FZ):
        site_z = site_z + (site >= float(k * FY * NF)).astype(F32)
    site = site - site_z * float(FY * NF)
    site_y = jnp.zeros((8, 128), F32)
    for k in range(1, FY):
        site_y = site_y + (site >= float(k * NF)).astype(F32)
    site_x = site - site_y * float(NF)
    own = whole_tile(width[0])
    offsets = offset[0, 0]
    for k, value in enumerate(
        (site_z, site_y, site_x, *(whole_tile(offsets[:, i : i + 1]) for i in range(3)), whole_tile(charge[0]))
    ):
        own = jnp.where(row8 == k, value, own)
    atoms[4] = own

    pl.semaphore_wait(barrier, len(greeted))

    neighbours = {}
    for dz in (-1, 1, 0):
        for dy in (-1, 1, 0):
            if (dz, dy) != (0, 0):
                slot = (1 - dz) * 3 + 1 - dy
                neighbours[slot] = pltpu.make_async_remote_copy(
                    atoms.at[4], atoms.at[slot], atom_send, atom_recv.at[2 * abs(dz) + abs(dy) - 1],
                    device_id=zy(dz, dy), device_id_type=MESH,
                )
    for copy in neighbours.values():
        copy.start()
    for dy in (-4, 4):
        greet(ring_z_ready, *zy(0, dy))
    for dz in (-8, 8):
        greet(ring_y_ready, *zy(dz, 0))

    plane_of = lax.broadcasted_iota(jnp.int32, (8, NC), 1)
    fine_of = lax.broadcasted_iota(jnp.int32, (8, NC), 0)
    away = plane_of - gz * (FZ // 2) - fine_of // 2
    away = jnp.where(away < 0, away + NC, away)
    odd = jnp.zeros((8, NC), F32)
    for shift, value in STENCIL:
        odd = jnp.where(away == shift % NC, value, odd)
    even = jnp.where(away == 0, 1.0, 0.0)
    along_z = jnp.where(fine_of % 2 == 1, odd, even)
    along_z = jnp.where(fine_of < FZ, along_z, 0.0).astype(BF16)
    loads[4].wait()
    for k in range(6):
        parts = split3(coarse[k])
        planes[k] = dot(along_z, parts[0]) + dot(along_z, parts[1]) + dot(along_z, parts[2])

    own_planes = planes.at[pl.ds(0, 6)]
    halos = [
        pltpu.make_async_remote_copy(
            own_planes, planes.at[pl.ds(6 * k, 6)], halo_send, halo_recv,
            device_id=zy(0, dy), device_id_type=MESH,
        )
        for k, dy in ((1, 1), (2, -1))
    ]
    for copy in halos:
        copy.start()

    lane128 = lax.broadcasted_iota(jnp.int32, (FZ, 128), 1)
    loads[5].wait()

    def put(y, low, high):
        if y < 8:
            field_0[pl.ds(y, FZ, stride=8), :] = low
            field_1[pl.ds(y, FZ, stride=8), :] = high
        else:
            for half in range(2):
                rows = pl.ds(40 + y + 4 * half, 3, stride=8)
                field_0[rows, :] = low[3 * half : 3 * half + 3]
                field_1[rows, :] = high[3 * half : 3 * half + 3]

    for pair in range(FY // 2):
        a, b, c = (density[:, 384 * pair + 128 * k : 384 * pair + 128 * k + 128] for k in range(3))
        rolled_b = pltpu.roll(b, 64, 1)
        rolled_c = pltpu.roll(c, 64, 1)
        put(2 * pair, a, b)
        put(2 * pair + 1, jnp.where(lane128 < 64, rolled_b, rolled_c), rolled_c)

    x = lax.broadcasted_iota(jnp.int32, (1, 256), 1).astype(F32)
    y_low = row8.astype(F32)
    y_high = jnp.where(row8 < 4, row8 + 8, row8 + 4).astype(F32)
    z = row8.astype(F32)

    def double(value):
        return jnp.concatenate([value, value], axis=1)

    upper = double(row8) < 4

    def charge_of(k):
        tile = atoms[k]
        dz, dy = k // 3 - 1, k % 3 - 1
        exponent = tile[7:8]
        wide = double(tile)
        from_z = (z - float(FZ * dz) - tile[0:1]) - tile[3:4]
        from_low = (y_low - float(FY * dy) - tile[1:2]) - tile[4:5]
        from_high = (y_high - float(FY * dy) - tile[1:2]) - tile[4:5]
        from_x = x - wide[2:3]
        from_x = jnp.where(from_x >= NF / 2, from_x - NF, from_x)
        from_x = jnp.where(from_x < -NF / 2, from_x + NF, from_x)
        from_x = from_x - wide[5:6]
        exp_z = double(jnp.exp(-exponent * (from_z * from_z)))
        exp_x = jnp.exp(-wide[7:8] * (from_x * from_x))
        low = double(jnp.exp(-exponent * (from_low * from_low))) * exp_x
        high = double(jnp.exp(-exponent * (from_high * from_high))) * exp_x
        floor = jnp.exp(-wide[7:8] * float(RC * RC))
        ratio = wide[7:8] / np.pi
        factor = wide[6:7] * (ratio * jnp.sqrt(ratio))
        powers = [low * exp_z[c : c + 1] for c in range(FZ)]
        powers += [high * jnp.where(upper, exp_z[c : c + 1], exp_z[c + 3 : c + 4]) for c in range(3)]
        return [factor * jnp.maximum(power - floor, 0.0) for power in powers]

    total = charge_of(4)

    group256 = double(group)

    def along_x_forward(values, store):
        count = values.shape[0]
        high, low = split2(values)
        both = jnp.concatenate([high, low], axis=0)
        for p in range(NY // 2):
            rep_h, rep_l = spans(p)
            out = dot(both, rep_h)
            out = out[:count] + (out[count:] + dot(high, rep_l))
            for i in range(count // 72):
                chosen = out[72 * i : 72 * i + 8]
                for g in range(1, 9):
                    chosen = jnp.where(group256 >= g, out[72 * i + 8 * g : 72 * i + 8 * g + 8], chosen)
                store(2 * p, i, chosen[:, :128])
                store(2 * p + 1, i, chosen[:, 128:])

    def history_along_x(first, count, send):
        def store(j, i, value):
            send[j, i] = value

        rows = slice(72 * first, 72 * (first + count))
        along_x_forward(jnp.concatenate([hist_0[rows, :], hist_1[rows, :]], axis=1), store)

    loads[7].wait()
    lane_h = lax.broadcasted_iota(jnp.int32, (HIST, 128), 1)
    for c in range(FZ):
        for pair in range(FY // 2):
            a, b, d = (history[c, :, 384 * pair + 128 * k : 384 * pair + 128 * k + 128] for k in range(3))
            rolled_b = pltpu.roll(b, 64, 1)
            rolled_d = pltpu.roll(d, 64, 1)
            for y, low, high in (
                (2 * pair, a, jnp.where(lane_h < 64, b, 0.0)),
                (2 * pair + 1, jnp.where(lane_h < 64, rolled_b, rolled_d), jnp.where(lane_h < 64, rolled_d, 0.0)),
            ):
                row = 8 * c + y if y < 8 else 48 + 8 * (c % 3) + 4 * (c // 3) + y - 8
                hist_0[pl.ds(row, HIST, stride=72), :] = low
                hist_1[pl.ds(row, HIST, stride=72), :] = high
    loads[6].wait()
    history_along_x(0, EARLY, send_g)

    whole = planes.at[pl.ds(0, 12)]
    pltpu.make_async_copy(whole, whole, halo_recv).wait()
    parts = split3(planes[...].reshape(144, NC))
    weights = table("ix")
    along_x = dot(parts[0], weights) + dot(parts[1], weights) + dot(parts[2], weights)
    parts = split3(along_x)
    weights = table("spread_y")
    smooth = dot(weights, parts[0]) + dot(weights, parts[1]) + dot(weights, parts[2])

    for kind, slots in ((0, (3, 5)), (1, (1, 7)), (2, (0, 2, 6, 8))):
        whole = atoms.at[pl.ds(0, len(slots))]
        pltpu.make_async_copy(whole, whole, atom_recv.at[kind]).wait()
        for k in slots:
            total = [a + b for a, b in zip(total, charge_of(k))]

    inside = lax.broadcasted_iota(jnp.int32, (8, 256), 1) < NF
    blocks = []
    for g in range(9):
        rows = slice(8 * g, 8 * g + 8)
        given = jnp.concatenate([field_0[rows, :], field_1[rows, :]], axis=1)
        value = jnp.where(inside, smooth[rows] + total[g] - given, 0.0)
        blocks.append(value)
        field_0[rows, :] = value[:, :128]
        field_1[rows, :] = value[:, 128:]

    def exchange_y(send, recv, ssem, rsem):
        def act(j):
            pltpu.make_async_remote_copy(
                send.at[j], recv.at[gy], ssem, rsem, device_id=(gz, j), device_id_type=MESH
            ).start()

        each_partner(gy, NY, act)
        recv[gy] = send[gy]
        whole = recv.at[pl.ds(0, NY - 1)]
        return pltpu.make_async_copy(whole, whole, rsem), pltpu.make_async_copy(whole, whole, ssem)

    def exchange_z(send, recv, ssem, rsem):
        mine = pl.ds(pl.multiple_of(gz * 8, 8), KY)

        def act(j):
            pltpu.make_async_remote_copy(
                send.at[pl.ds(pl.multiple_of(j * 8, 8), KY)], recv.at[mine],
                ssem, rsem, device_id=(j, gy), device_id_type=MESH,
            ).start()

        each_partner(gz, NZ, act)
        recv[mine, :] = send[mine, :]
        whole = recv.at[pl.ds(0, KY * (NZ - 1))]
        return pltpu.make_async_copy(whole, whole, rsem), pltpu.make_async_copy(whole, whole, ssem)

    def store_residual(j, i, value):
        send1[j] = value

    along_x_forward(jnp.concatenate(blocks, axis=0), store_residual)
    pl.semaphore_wait(ring_z_ready, 2)
    arrived, sent1 = exchange_y(send1, recv1, s1, r1)
    arrived_g, sent_g = exchange_y(send_g, recv_g, sg, rg)
    pl.semaphore_wait(ring_y_ready, 2)
    for j in ring_x:
        greet(plane_ready, j, gy)
    history_along_x(EARLY, HIST - EARLY, send_h)

    groups128 = jnp.concatenate([group] * NY, axis=0)
    rows128 = jnp.concatenate([row8] * NY, axis=0)
    from_upper = (groups128 < 3) & (rows128 < 4)
    from_lower = (groups128 >= 3) & (groups128 < 6) & (rows128 >= 4)
    arrived.wait()
    packed = recv1[...].reshape(128, 128)
    moved = jnp.where(
        from_upper, pltpu.roll(packed, 128 - 72, 1), jnp.where(from_lower, pltpu.roll(packed, 128 - 36, 1), 0.0)
    )
    send2[...] = dot3((table("fy_h"), table("fy_l")), split2(jnp.concatenate([packed, moved], axis=0)))
    pl.semaphore_wait(plane_ready, 3)
    arrived, sent2 = exchange_z(send2, recv2, s2, r2)
    arrived_h, sent_h = exchange_y(send_h, recv_h, sh, rh)

    def give(out, first, second):
        for pair in range(FY // 2):
            if pair < 4:
                places = ((0, FZ, 2 * pair),)
            else:
                places = ((0, 3, 40 + 2 * pair), (3, 3, 44 + 2 * pair))
            for top, count, row in places:
                low_lanes = lax.broadcasted_iota(jnp.int32, (count, 128), 1) < 64
                a = first[pl.ds(row, count, stride=8), :]
                b = second[pl.ds(row, count, stride=8), :]
                c = pltpu.roll(first[pl.ds(row + 1, count, stride=8), :], 64, 1)
                d = pltpu.roll(second[pl.ds(row + 1, count, stride=8), :], 64, 1)
                tiles = (a, jnp.where(low_lanes, b, c), jnp.where(low_lanes, c, d))
                for k, tile in enumerate(tiles):
                    out[top : top + count, 384 * pair + 128 * k : 384 * pair + 128 * k + 128] = tile

    give(residual_out, field_0, field_1)
    arrived.wait()

    group1 = group[0:1]

    def swapped(pieces, position):
        result = None
        for b in range(6):
            shift = (KX * (b - position)) % 128
            moved = pltpu.roll(pieces[b], shift, 1) if shift else pieces[b]
            result = moved if result is None else jnp.where(group1 >= b, moved, result)
        return result

    pieces = [recv2[pl.ds(b, NZ, stride=8), :] for b in range(KY)]
    stacked = jnp.concatenate([swapped(pieces, a) for a in range(FZ)], axis=0)
    spectrum = dot3((table("fz_h"), table("fz_l")), split2(stacked)) * weight[...]
    back = dot3((table("gz_h"), table("gz_l")), split2(spectrum))
    pieces = [back[NZ * a : NZ * a + NZ] for a in range(FZ)]
    for b in range(KY):
        send4[pl.ds(b, NZ, stride=8), :] = swapped(pieces, b)
    arrived, sent4 = exchange_z(send4, recv4, s4, r4)
    arrived.wait()

    rows256 = jnp.concatenate([rows128, rows128], axis=0)
    out = dot3((table("gy_h"), table("gy_l")), split2(jnp.where(rows256 < KY, recv4[0:256, :], 0.0)))
    low, high = out[:128], out[128:]
    packed = jnp.where(
        groups128 < 6, low, jnp.where(rows128 < 4, pltpu.roll(high, 72, 1), pltpu.roll(high, 36, 1))
    )
    arrived_g.wait()
    arrived_h.wait()
    terms = [jnp.zeros((8, 128), F32) for _ in range(HIST + 1)]
    for j in range(NY):
        tile = jnp.where(group < 9, packed[8 * j : 8 * j + 8], 0.0)
        for i in range(EARLY):
            terms[i] = terms[i] + recv_g[j, i] * tile
        for i in range(EARLY, HIST):
            terms[i] = terms[i] + recv_h[j, i - EARLY] * tile
        terms[HIST] = terms[HIST] + recv1[j] * tile
    rows = jnp.concatenate(
        [jnp.sum(t, axis=0, keepdims=True) for t in terms] + [jnp.zeros((7, 128), F32)], axis=0
    ) * (1.0 / float(NF) ** 3)
    column = jnp.sum(rows, axis=1, keepdims=True)
    lane_of = lax.broadcasted_iota(jnp.int32, (16, 128), 1)
    row_of = lax.broadcasted_iota(jnp.int32, (16, 128), 0)
    line = jnp.sum(jnp.where(lane_of == row_of, column, 0.0), axis=0, keepdims=True)

    row_b[gz] = line

    def act_b(j):
        pltpu.make_async_remote_copy(
            row_b.at[gz], row_b.at[gz], sb, rb, device_id=(j, gy), device_id_type=MESH
        ).start()

    each_partner(gz, NZ, act_b)
    for j in range(NY):
        send5[j] = packed[8 * j : 8 * j + 8]
    arrived, sent5 = exchange_y(send5, recv5, s5, r5)
    whole_b = row_b.at[pl.ds(0, NZ - 1)]
    pltpu.make_async_copy(whole_b, whole_b, rb).wait()
    row_a[gy] = jnp.sum(row_b[...], axis=0)

    def act_a(j):
        pltpu.make_async_remote_copy(
            row_a.at[gy], row_a.at[gy], sa, ra, device_id=(gz, j), device_id_type=MESH
        ).start()

    each_partner(gy, NY, act_a)

    arrived.wait()
    potential = jnp.zeros((72, 256), F32)
    for p in range(NY // 2):
        pair = split2(jnp.concatenate([recv5[2 * p], recv5[2 * p + 1]], axis=1))
        masked = [
            jnp.concatenate([jnp.where(group256 == g, part.astype(F32), 0.0) for g in range(9)], axis=0).astype(BF16)
            for part in pair
        ]
        potential = potential + dot3(masked, spans(p), dot_nt)
    out_0[0:72, :] = potential[:, :128]
    out_1[0:72, :] = potential[:, 128:]
    give(potential_out, out_0, out_1)

    whole_a = row_a.at[pl.ds(0, NY - 1)]
    pltpu.make_async_copy(whole_a, whole_a, ra).wait()
    sums_out[...] = jnp.sum(row_a[...], axis=0)[0, : HIST + 1]

    whole = atoms.at[pl.ds(0, 8)]
    pltpu.make_async_copy(whole, whole, atom_send).wait()
    whole = planes.at[pl.ds(0, 12)]
    pltpu.make_async_copy(whole, whole, halo_send).wait()
    for copy in (sent1, sent2, sent_g, sent_h, sent4, sent5):
        copy.wait()
    pltpu.make_async_copy(whole_a, whole_a, sa).wait()
    pltpu.make_async_copy(whole_b, whole_b, sb).wait()


def write_out(*refs):
    copies = [pltpu.make_async_copy(refs[k], refs[3 + k], refs[6].at[k]) for k in range(3)]
    for copy in copies:
        copy.start()
    for copy in copies:
        copy.wait()


def solution(mesh):
    constants, place = tables()

    def local(coarse, density, history, cell, offset, charge, width):
        coarse = jnp.transpose(coarse, (1, 0, 2))
        history = jnp.transpose(history, (1, 0, 2))
        offset = jnp.transpose(offset, (1, 2, 3, 0))
        inputs = (cell, offset, charge, width, coarse, density, history)
        inputs = (*inputs, jnp.asarray(constants))
        vmem = pl.BlockSpec(memory_space=pltpu.VMEM)
        dma = pltpu.SemaphoreType.DMA
        tile = (NY, 8, 128)
        residual, potential, sums = pl.pallas_call(
            functools.partial(kernel, place),
            out_shape=(
                pltpu.VMEM((FZ, FY * NF), F32),
                pltpu.VMEM((FZ, FY * NF), F32),
                pltpu.VMEM((HIST + 1,), F32),
            ),
            in_specs=[pl.BlockSpec(memory_space=pltpu.HBM)] * len(inputs),
            out_specs=(vmem, vmem, vmem),
            scratch_shapes=[
                *(pltpu.VMEM(i.shape, i.dtype) for i in inputs),
                pltpu.VMEM((18, 8, NC), F32),
                pltpu.VMEM((9, 8, 128), F32),
                *[pltpu.VMEM((128, 128), F32)] * 4,
                *[pltpu.VMEM((648, 128), F32)] * 2,
                *[pltpu.VMEM(tile, F32)] * 2,
                pltpu.VMEM((256, 128), F32),
                *[pltpu.VMEM((264, 128), F32)] * 3,
                *[pltpu.VMEM(tile, F32)] * 2,
                *[pltpu.VMEM((NY, EARLY, 8, 128), F32)] * 2,
                *[pltpu.VMEM((NY, HIST - EARLY, 8, 128), F32)] * 2,
                pltpu.VMEM((NF, 128), F32),
                pltpu.VMEM((NY, 1, 128), F32),
                pltpu.VMEM((NZ, 1, 128), F32),
                dma((8,)), dma, dma, dma, dma((3,)),
                *[dma] * 16,
                *[pltpu.SemaphoreType.REGULAR] * 3,
            ],
            compiler_params=pltpu.CompilerParams(collective_id=0, has_side_effects=True),
        )(*inputs)
        results = tuple(pltpu.with_memory_space_constraint(r, pltpu.VMEM) for r in (residual, potential, sums))
        hbm = pl.BlockSpec(memory_space=pltpu.HBM)
        return pl.pallas_call(
            write_out,
            out_shape=tuple(jax.ShapeDtypeStruct(r.shape, F32) for r in results),
            in_specs=[vmem] * 3,
            out_specs=(hbm,) * 3,
            scratch_shapes=[dma((3,))],
        )(*results)

    in_specs = (
        P(None, "gy", None),
        P("gz", "gy"),
        P(None, "gz", "gy"),
        P("gz", "gy", None),
        P(None, "gz", "gy", None),
        P("gz", "gy", None),
        P("gz", "gy", None),
    )
    out_specs = (P("gz", "gy"), P("gz", "gy"), P())
    return jax.shard_map(local, mesh=mesh, in_specs=in_specs, out_specs=out_specs, check_vma=False)
```

```python
import functools

import jax
import jax.numpy as jnp
import numpy as np
from jax import lax
from jax.experimental import pallas as pl
from jax.experimental.pallas import tpu as pltpu
from jax.sharding import PartitionSpec as P

MESH = pl.DeviceIdType.MESH
NC = 96
NF = 192
HIST = 8
EARLY = 3
RC = 4
FZ = 6
FY = 12
NZ = 32
NY = 16
KX = NF // NY
KY = NF // NZ
STENCIL = ((-1, -1.0 / 16.0), (0, 9.0 / 16.0), (1, 9.0 / 16.0), (2, -1.0 / 16.0))
F32 = jnp.float32
BF16 = jnp.bfloat16


def two(table):
    high = np.asarray(table, np.float32).astype(jnp.bfloat16)
    low = (table - high.astype(np.float64)).astype(np.float32).astype(jnp.bfloat16)
    return high, low


def hartley():
    n = np.arange(NF)
    angle = 2.0 * np.pi / NF * (n[:, None] * n[None, :] % NF)
    return (np.cos(angle) + np.sin(angle)) / np.sqrt(NF)


def tables():
    h = hartley()
    rep = np.zeros((256, NY, 128))
    for j in range(NY):
        for g in range(9):
            rep[:NF, j, g * KX : (g + 1) * KX] = h[:, j * KX : (j + 1) * KX]
    rep = rep.reshape(256, NY * 128)
    by_y = h.reshape(NZ, KY, NY, FY)
    fy = np.zeros((NZ, 8, 2, NY, 8))
    fy[:, :KY, 0] = by_y[:, :, :, :8]
    fy[:, :KY, 1, :, :4] = by_y[:, :, :, 8:]
    fy[:, :KY, 1, :, 4:] = by_y[:, :, :, 8:]
    fy = fy.reshape(256, 256)
    fz = h.reshape(NF, NZ, FZ).transpose(0, 2, 1).reshape(NF, NF)
    ix = np.zeros((256, NC))
    for i in range(NC):
        ix[2 * i, i] = 1.0
        for offset, value in STENCIL:
            ix[2 * i + 1, (i + offset) % NC] += value
    wy = np.zeros((FY, FY // 2 + 3))
    for i in range(FY // 2):
        wy[2 * i, i + 1] = 1.0
        for offset, value in STENCIL:
            wy[2 * i + 1, i + 1 + offset] += value
    place = [(1, 5)] + [(0, r) for r in range(6)] + [(2, 0), (2, 1)]
    spread_y = np.zeros((72, 3, 6, 8))
    for z in range(FZ):
        for y in range(FY):
            row = 8 * z + y if y < 8 else 48 + 8 * (z % 3) + 4 * (z // 3) + y - 8
            for r, (block, coarse_y) in enumerate(place):
                spread_y[row, block, coarse_y, z] = wy[y, r]
    exact = [t.astype(np.float32).astype(jnp.bfloat16) for t in (ix.T, spread_y.reshape(72, 144))]
    pieces = {"ix": exact[0], "spread_y": exact[1]}
    for name, table in (("fy", fy), ("gy", fy.T), ("fz", fz), ("gz", fz.T)):
        pieces[name + "_h"], pieces[name + "_l"] = two(table)
    by_span = rep.reshape(256, NY // 2, 256).transpose(1, 0, 2).reshape(-1, 256)
    pieces["rep_h"], pieces["rep_l"] = two(by_span)
    place, stack, row = {}, [], 0
    for name, piece in pieces.items():
        rows, columns = piece.shape
        place[name] = (row, rows, columns)
        stack.append(np.pad(piece, ((0, -rows % 16), (0, 256 - columns))))
        row += rows + -rows % 16
    return np.concatenate(stack, axis=0), place


def split2(value):
    high = value.astype(BF16)
    return high, (value - high.astype(F32)).astype(BF16)


def split3(value):
    high = value.astype(BF16)
    rest = value - high.astype(F32)
    middle = rest.astype(BF16)
    return high, middle, (rest - middle.astype(F32)).astype(BF16)


def dot(a, b):
    return jnp.dot(a, b, preferred_element_type=F32)


def dot_nt(a, b):
    return lax.dot_general(a, b, (((1,), (1,)), ((), ())), preferred_element_type=F32)


def dot3(a, b, product=dot):
    return product(a[0], b[0]) + product(a[1], b[0]) + product(a[0], b[1])


def dot_data(table, value):
    high, low = split2(value)
    width = value.shape[1]
    both = dot(table[0], jnp.concatenate([high, low], axis=1))
    return both[:, :width] + (both[:, width:] + dot(table[1], high))


def wrap(index, count):
    return jnp.where(index >= count, index - count, index)


def each_partner(me, count, act):
    act(wrap(me + count // 2, count))

    def body(t, _):
        act(wrap(me + count // 2 - t, count))
        act(wrap(me + count // 2 + t, count))
        return 0

    lax.fori_loop(1, count // 2, body, 0, unroll=True)


def kernel(
    place, cell_in, offset_in, charge_in, width_in, coarse_in, density_in, history_in, tables_in, *refs
):
    residual_out, potential_out, sums_out = refs[:3]
    (
        cell, offset, charge, width, coarse, density, history, all_tables,
        planes, atoms, field_0, field_1, out_0, out_1, hist_0, hist_1,
        send1, recv1, send2, recv2, send4, recv4, send5, recv5, send_g, recv_g, send_h, recv_h,
        weight, row_a, row_b,
        load_sem, halo_send, halo_recv, atom_send, atom_recv,
        s1, r1, s2, r2, s4, r4, s5, r5, sg, rg, sh, rh, sa, ra, sb, rb, ring_z_ready, ring_y_ready, plane_ready,
    ) = refs[3:]
    gz = lax.axis_index("gz")
    gy = lax.axis_index("gy")

    def zy(dz, dy):
        return (wrap(wrap(gz + dz + NZ, NZ), NZ) if dz else gz, wrap(wrap(gy + dy + NY, NY), NY) if dy else gy)

    barrier = pltpu.get_barrier_semaphore()

    def greet(semaphore, z, y):
        pl.semaphore_signal(semaphore, inc=1, device_id=(z, y), device_id_type=MESH)

    column = lax.rem(gz, 4)
    ring_x = [gz - column + lax.rem(column + k, 4) for k in (2, 1, 3)]
    other_core = gy + 1 - 2 * lax.rem(gy, 2)
    greeted = [zy(dz, dy) for dz in (-1, 1) for dy in (-1, 1)]
    greeted += [zy(dz, 0) for dz in (-8, 8)] + [(j, gy) for j in ring_x]
    greeted += [(gz, wrap(wrap(core + dy + NY, NY), NY)) for dy in (-4, 4, -2, 2) for core in (gy, other_core)]
    greeted += [zy(dz, 0) for dz in (-4, 4, -1, 1)] + [(gz, other_core)]
    for z, y in greeted:
        greet(barrier, z, y)

    sources = (
        cell_in, offset_in, charge_in, width_in, coarse_in, density_in, tables_in, history_in,
    )
    targets = (cell, offset, charge, width, coarse, density, all_tables, history)
    loads = {}
    for k, (source, target) in enumerate(zip(sources, targets)):
        loads[k] = pltpu.make_async_copy(source, target, load_sem.at[k])
        loads[k].start()

    def table(name):
        row, rows, columns = place[name]
        return all_tables[row : row + rows, :columns]

    def spans(p):
        return tuple(
            all_tables[place[name][0] + 256 * p : place[name][0] + 256 * p + 256, :]
            for name in ("rep_h", "rep_l")
        )

    row8 = lax.broadcasted_iota(jnp.int32, (8, 128), 0)
    lane8 = lax.broadcasted_iota(jnp.int32, (8, 128), 1)
    group = jnp.zeros_like(lane8)
    for c in range(1, 11):
        group = group + (lane8 >= c * KX).astype(jnp.int32)

    def square(counter):
        wave = jnp.where(counter < NF // 2, counter, counter - NF)
        return wave * wave

    wave_yx = (square(gz * KY + group) + square(gy * KX + lane8 - KX * group))[0:1]
    used = (lane8 < KY * KX)[0:1]
    squares = square(lax.broadcasted_iota(jnp.int32, (NF, 128), 0)) + wave_yx
    scaled = (2.0 * np.pi / NF) ** 2 * jnp.maximum(squares, 1).astype(F32)
    weight[...] = jnp.where((squares > 0) & used, 4.0 * np.pi / scaled, 0.0)

    for k in range(4):
        loads[k].wait()

    def whole_tile(value):
        return jnp.broadcast_to(value, (8, 128))

    site = whole_tile(cell[0].astype(F32))
    site_z = jnp.zeros((8, 128), F32)
    for k in range(1, FZ):
        site_z = site_z + (site >= float(k * FY * NF)).astype(F32)
    site = site - site_z * float(FY * NF)
    site_y = jnp.zeros((8, 128), F32)
    for k in range(1, FY):
        site_y = site_y + (site >= float(k * NF)).astype(F32)
    site_x = site - site_y * float(NF)
    own = whole_tile(width[0])
    offsets = offset[0, 0]
    for k, value in enumerate(
        (site_z, site_y, site_x, *(whole_tile(offsets[:, i : i + 1]) for i in range(3)), whole_tile(charge[0]))
    ):
        own = jnp.where(row8 == k, value, own)
    atoms[4] = own

    pl.semaphore_wait(barrier, len(greeted))

    neighbours = {}
    for dz in (-1, 1, 0):
        for dy in (-1, 1, 0):
            if (dz, dy) != (0, 0):
                slot = (1 - dz) * 3 + 1 - dy
                neighbours[slot] = pltpu.make_async_remote_copy(
                    atoms.at[4], atoms.at[slot], atom_send, atom_recv.at[2 * abs(dz) + abs(dy) - 1],
                    device_id=zy(dz, dy), device_id_type=MESH,
                )
    for copy in neighbours.values():
        copy.start()
    for dy in (-4, 4):
        greet(ring_z_ready, *zy(0, dy))
    for dz in (-8, 8):
        greet(ring_y_ready, *zy(dz, 0))

    plane_of = lax.broadcasted_iota(jnp.int32, (8, NC), 1)
    fine_of = lax.broadcasted_iota(jnp.int32, (8, NC), 0)
    away = plane_of - gz * (FZ // 2) - fine_of // 2
    away = jnp.where(away < 0, away + NC, away)
    odd = jnp.zeros((8, NC), F32)
    for shift, value in STENCIL:
        odd = jnp.where(away == shift % NC, value, odd)
    even = jnp.where(away == 0, 1.0, 0.0)
    along_z = jnp.where(fine_of % 2 == 1, odd, even)
    along_z = jnp.where(fine_of < FZ, along_z, 0.0).astype(BF16)
    loads[4].wait()
    for k in range(6):
        parts = split3(coarse[k])
        planes[k] = dot(along_z, parts[0]) + dot(along_z, parts[1]) + dot(along_z, parts[2])

    own_planes = planes.at[pl.ds(0, 6)]
    halos = [
        pltpu.make_async_remote_copy(
            own_planes, planes.at[pl.ds(6 * k, 6)], halo_send, halo_recv,
            device_id=zy(0, dy), device_id_type=MESH,
        )
        for k, dy in ((1, 1), (2, -1))
    ]
    for copy in halos:
        copy.start()

    lane128 = lax.broadcasted_iota(jnp.int32, (FZ, 128), 1)
    loads[5].wait()

    def put(y, low, high):
        if y < 8:
            field_0[pl.ds(y, FZ, stride=8), :] = low
            field_1[pl.ds(y, FZ, stride=8), :] = high
        else:
            for half in range(2):
                rows = pl.ds(40 + y + 4 * half, 3, stride=8)
                field_0[rows, :] = low[3 * half : 3 * half + 3]
                field_1[rows, :] = high[3 * half : 3 * half + 3]

    for pair in range(FY // 2):
        a, b, c = (density[:, 384 * pair + 128 * k : 384 * pair + 128 * k + 128] for k in range(3))
        rolled_b = pltpu.roll(b, 64, 1)
        rolled_c = pltpu.roll(c, 64, 1)
        put(2 * pair, a, b)
        put(2 * pair + 1, jnp.where(lane128 < 64, rolled_b, rolled_c), rolled_c)

    x = lax.broadcasted_iota(jnp.int32, (1, 256), 1).astype(F32)
    y_low = row8.astype(F32)
    y_high = jnp.where(row8 < 4, row8 + 8, row8 + 4).astype(F32)
    z = row8.astype(F32)

    def double(value):
        return jnp.concatenate([value, value], axis=1)

    upper = double(row8) < 4

    def charge_of(k):
        tile = atoms[k]
        dz, dy = k // 3 - 1, k % 3 - 1
        exponent = tile[7:8]
        wide = double(tile)
        from_z = (z - float(FZ * dz) - tile[0:1]) - tile[3:4]
        from_low = (y_low - float(FY * dy) - tile[1:2]) - tile[4:5]
        from_high = (y_high - float(FY * dy) - tile[1:2]) - tile[4:5]
        from_x = x - wide[2:3]
        from_x = jnp.where(from_x >= NF / 2, from_x - NF, from_x)
        from_x = jnp.where(from_x < -NF / 2, from_x + NF, from_x)
        from_x = from_x - wide[5:6]
        exp_z = double(jnp.exp(-exponent * (from_z * from_z)))
        exp_x = jnp.exp(-wide[7:8] * (from_x * from_x))
        low = double(jnp.exp(-exponent * (from_low * from_low))) * exp_x
        high = double(jnp.exp(-exponent * (from_high * from_high))) * exp_x
        floor = jnp.exp(-wide[7:8] * float(RC * RC))
        ratio = wide[7:8] / np.pi
        factor = wide[6:7] * (ratio * jnp.sqrt(ratio))
        powers = [low * exp_z[c : c + 1] for c in range(FZ)]
        powers += [high * jnp.where(upper, exp_z[c : c + 1], exp_z[c + 3 : c + 4]) for c in range(3)]
        return [factor * jnp.maximum(power - floor, 0.0) for power in powers]

    total = charge_of(4)

    group256 = double(group)

    def along_x_forward(values, store):
        count = values.shape[0]
        high, low = split2(values)
        both = jnp.concatenate([high, low], axis=0)
        for p in range(NY // 2):
            rep_h, rep_l = spans(p)
            out = dot(both, rep_h)
            out = out[:count] + (out[count:] + dot(high, rep_l))
            for i in range(count // 72):
                chosen = out[72 * i : 72 * i + 8]
                for g in range(1, 9):
                    chosen = jnp.where(group256 >= g, out[72 * i + 8 * g : 72 * i + 8 * g + 8], chosen)
                store(2 * p, i, chosen[:, :128])
                store(2 * p + 1, i, chosen[:, 128:])

    def history_along_x(first, count, send):
        def store(j, i, value):
            send[j, i] = value

        rows = slice(72 * first, 72 * (first + count))
        along_x_forward(jnp.concatenate([hist_0[rows, :], hist_1[rows, :]], axis=1), store)

    loads[7].wait()
    lane_h = lax.broadcasted_iota(jnp.int32, (HIST, 128), 1)
    for c in range(FZ):
        for pair in range(FY // 2):
            a, b, d = (history[c, :, 384 * pair + 128 * k : 384 * pair + 128 * k + 128] for k in range(3))
            rolled_b = pltpu.roll(b, 64, 1)
            rolled_d = pltpu.roll(d, 64, 1)
            for y, low, high in (
                (2 * pair, a, jnp.where(lane_h < 64, b, 0.0)),
                (2 * pair + 1, jnp.where(lane_h < 64, rolled_b, rolled_d), jnp.where(lane_h < 64, rolled_d, 0.0)),
            ):
                row = 8 * c + y if y < 8 else 48 + 8 * (c % 3) + 4 * (c // 3) + y - 8
                hist_0[pl.ds(row, HIST, stride=72), :] = low
                hist_1[pl.ds(row, HIST, stride=72), :] = high
    loads[6].wait()
    history_along_x(0, EARLY, send_g)

    whole = planes.at[pl.ds(0, 12)]
    pltpu.make_async_copy(whole, whole, halo_recv).wait()
    parts = split3(planes[...].reshape(144, NC))
    weights = table("ix")
    along_x = dot(parts[0], weights) + dot(parts[1], weights) + dot(parts[2], weights)
    parts = split3(along_x)
    weights = table("spread_y")
    smooth = dot(weights, parts[0]) + dot(weights, parts[1]) + dot(weights, parts[2])

    for kind, slots in ((0, (3, 5)), (1, (1, 7)), (2, (0, 2, 6, 8))):
        whole = atoms.at[pl.ds(0, len(slots))]
        pltpu.make_async_copy(whole, whole, atom_recv.at[kind]).wait()
        for k in slots:
            total = [a + b for a, b in zip(total, charge_of(k))]

    inside = lax.broadcasted_iota(jnp.int32, (8, 256), 1) < NF
    blocks = []
    for g in range(9):
        rows = slice(8 * g, 8 * g + 8)
        given = jnp.concatenate([field_0[rows, :], field_1[rows, :]], axis=1)
        value = jnp.where(inside, smooth[rows] + total[g] - given, 0.0)
        blocks.append(value)
        field_0[rows, :] = value[:, :128]
        field_1[rows, :] = value[:, 128:]

    def exchange_y(send, recv, ssem, rsem):
        def act(j):
            pltpu.make_async_remote_copy(
                send.at[j], recv.at[gy], ssem, rsem, device_id=(gz, j), device_id_type=MESH
            ).start()

        each_partner(gy, NY, act)
        recv[gy] = send[gy]
        whole = recv.at[pl.ds(0, NY - 1)]
        return pltpu.make_async_copy(whole, whole, rsem), pltpu.make_async_copy(whole, whole, ssem)

    def exchange_z(send, recv, ssem, rsem):
        mine = pl.ds(pl.multiple_of(gz * 8, 8), KY)

        def act(j):
            pltpu.make_async_remote_copy(
                send.at[pl.ds(pl.multiple_of(j * 8, 8), KY)], recv.at[mine],
                ssem, rsem, device_id=(j, gy), device_id_type=MESH,
            ).start()

        each_partner(gz, NZ, act)
        recv[mine, :] = send[mine, :]
        whole = recv.at[pl.ds(0, KY * (NZ - 1))]
        return pltpu.make_async_copy(whole, whole, rsem), pltpu.make_async_copy(whole, whole, ssem)

    pl.semaphore_wait(ring_z_ready, 2)
    high, low = split2(jnp.concatenate(blocks, axis=0))
    both = jnp.concatenate([high, low], axis=0)
    chip = gy // 2
    for part in ((4, 3, 5), (2, 6, 1, 7, 0)):
        done = []
        for away in part:
            p = wrap(chip + away, NY // 2)
            rows = [
                all_tables[pl.ds(pl.multiple_of(place[name][0] + 256 * p, 16), 256), :]
                for name in ("rep_h", "rep_l")
            ]
            out = dot(both, rows[0])
            out = out[:72] + (out[72:] + dot(high, rows[1]))
            chosen = out[0:8]
            for g in range(1, 9):
                chosen = jnp.where(group256 >= g, out[8 * g : 8 * g + 8], chosen)
            done.append((away, p, chosen))
        for away, p, chosen in done:
            send1[2 * p] = chosen[:, :128]
            send1[2 * p + 1] = chosen[:, 128:]
        for away, p, _ in done:
            for j in (2 * p, 2 * p + 1) if away else (other_core,):
                pltpu.make_async_remote_copy(
                    send1.at[j], recv1.at[gy], s1, r1, device_id=(gz, j), device_id_type=MESH
                ).start()
    recv1[gy] = send1[gy]
    whole = recv1.at[pl.ds(0, NY - 1)]
    arrived = pltpu.make_async_copy(whole, whole, r1)
    sent1 = pltpu.make_async_copy(whole, whole, s1)
    arrived_g, sent_g = exchange_y(send_g, recv_g, sg, rg)
    pl.semaphore_wait(ring_y_ready, 2)
    for j in ring_x:
        greet(plane_ready, j, gy)
    history_along_x(EARLY, HIST - EARLY, send_h)
    arrived_h, sent_h = exchange_y(send_h, recv_h, sh, rh)

    groups128 = jnp.concatenate([group] * NY, axis=0)
    rows128 = jnp.concatenate([row8] * NY, axis=0)
    from_upper = (groups128 < 3) & (rows128 < 4)
    from_lower = (groups128 >= 3) & (groups128 < 6) & (rows128 >= 4)
    arrived.wait()
    packed = recv1[...].reshape(128, 128)
    moved = jnp.where(
        from_upper, pltpu.roll(packed, 128 - 72, 1), jnp.where(from_lower, pltpu.roll(packed, 128 - 36, 1), 0.0)
    )
    send2[...] = dot_data((table("fy_h"), table("fy_l")), (jnp.concatenate([packed, moved], axis=0)))
    pl.semaphore_wait(plane_ready, 3)
    arrived, sent2 = exchange_z(send2, recv2, s2, r2)

    def give(out, first, second):
        for pair in range(FY // 2):
            if pair < 4:
                places = ((0, FZ, 2 * pair),)
            else:
                places = ((0, 3, 40 + 2 * pair), (3, 3, 44 + 2 * pair))
            for top, count, row in places:
                low_lanes = lax.broadcasted_iota(jnp.int32, (count, 128), 1) < 64
                a = first[pl.ds(row, count, stride=8), :]
                b = second[pl.ds(row, count, stride=8), :]
                c = pltpu.roll(first[pl.ds(row + 1, count, stride=8), :], 64, 1)
                d = pltpu.roll(second[pl.ds(row + 1, count, stride=8), :], 64, 1)
                tiles = (a, jnp.where(low_lanes, b, c), jnp.where(low_lanes, c, d))
                for k, tile in enumerate(tiles):
                    out[top : top + count, 384 * pair + 128 * k : 384 * pair + 128 * k + 128] = tile

    give(residual_out, field_0, field_1)
    arrived.wait()

    group1 = group[0:1]

    def swapped(pieces, position):
        result = None
        for b in range(6):
            shift = (KX * (b - position)) % 128
            moved = pltpu.roll(pieces[b], shift, 1) if shift else pieces[b]
            result = moved if result is None else jnp.where(group1 >= b, moved, result)
        return result

    pieces = [recv2[pl.ds(b, NZ, stride=8), :] for b in range(KY)]
    stacked = jnp.concatenate([swapped(pieces, a) for a in range(FZ)], axis=0)
    spectrum = dot_data((table("fz_h"), table("fz_l")), (stacked)) * weight[...]
    back = dot_data((table("gz_h"), table("gz_l")), (spectrum))
    pieces = [back[NZ * a : NZ * a + NZ] for a in range(FZ)]
    for b in range(KY):
        send4[pl.ds(b, NZ, stride=8), :] = swapped(pieces, b)
    arrived, sent4 = exchange_z(send4, recv4, s4, r4)
    arrived.wait()

    rows256 = jnp.concatenate([rows128, rows128], axis=0)
    out = dot_data((table("gy_h"), table("gy_l")), (jnp.where(rows256 < KY, recv4[0:256, :], 0.0)))
    low, high = out[:128], out[128:]
    packed = jnp.where(
        groups128 < 6, low, jnp.where(rows128 < 4, pltpu.roll(high, 72, 1), pltpu.roll(high, 36, 1))
    )
    arrived_g.wait()
    arrived_h.wait()
    terms = [jnp.zeros((8, 128), F32) for _ in range(HIST + 1)]
    for j in range(NY):
        tile = jnp.where(group < 9, packed[8 * j : 8 * j + 8], 0.0)
        for i in range(EARLY):
            terms[i] = terms[i] + recv_g[j, i] * tile
        for i in range(EARLY, HIST):
            terms[i] = terms[i] + recv_h[j, i - EARLY] * tile
        terms[HIST] = terms[HIST] + recv1[j] * tile
    rows = jnp.concatenate(
        [jnp.sum(t, axis=0, keepdims=True) for t in terms] + [jnp.zeros((7, 128), F32)], axis=0
    ) * (1.0 / float(NF) ** 3)
    column = jnp.sum(rows, axis=1, keepdims=True)
    lane_of = lax.broadcasted_iota(jnp.int32, (16, 128), 1)
    row_of = lax.broadcasted_iota(jnp.int32, (16, 128), 0)
    line = jnp.sum(jnp.where(lane_of == row_of, column, 0.0), axis=0, keepdims=True)

    row_b[gz] = line

    def act_b(j):
        pltpu.make_async_remote_copy(
            row_b.at[gz], row_b.at[gz], sb, rb, device_id=(j, gy), device_id_type=MESH
        ).start()

    each_partner(gz, NZ, act_b)
    for j in range(NY):
        send5[j] = packed[8 * j : 8 * j + 8]
    arrived, sent5 = exchange_y(send5, recv5, s5, r5)
    whole_b = row_b.at[pl.ds(0, NZ - 1)]
    pltpu.make_async_copy(whole_b, whole_b, rb).wait()
    row_a[gy] = jnp.sum(row_b[...], axis=0)

    def act_a(j):
        pltpu.make_async_remote_copy(
            row_a.at[gy], row_a.at[gy], sa, ra, device_id=(gz, j), device_id_type=MESH
        ).start()

    each_partner(gy, NY, act_a)

    arrived.wait()
    potential = jnp.zeros((72, 256), F32)
    for p in range(NY // 2):
        pair = split2(jnp.concatenate([recv5[2 * p], recv5[2 * p + 1]], axis=1))
        masked = [
            jnp.concatenate([jnp.where(group256 == g, part.astype(F32), 0.0) for g in range(9)], axis=0).astype(BF16)
            for part in pair
        ]
        potential = potential + dot3(masked, spans(p), dot_nt)
    out_0[0:72, :] = potential[:, :128]
    out_1[0:72, :] = potential[:, 128:]
    give(potential_out, out_0, out_1)

    whole = atoms.at[pl.ds(0, 8)]
    pltpu.make_async_copy(whole, whole, atom_send).wait()
    whole = planes.at[pl.ds(0, 12)]
    pltpu.make_async_copy(whole, whole, halo_send).wait()
    for copy in (sent1, sent2, sent_g, sent_h, sent4, sent5):
        copy.wait()
    pltpu.make_async_copy(whole_b, whole_b, sb).wait()
    whole_a = row_a.at[pl.ds(0, NY - 1)]
    pltpu.make_async_copy(whole_a, whole_a, sa).wait()
    pltpu.make_async_copy(whole_a, whole_a, ra).wait()
    sums_out[...] = jnp.sum(row_a[...], axis=0)[0, : HIST + 1]


def write_out(*refs):
    copies = [pltpu.make_async_copy(refs[k], refs[3 + k], refs[6].at[k]) for k in range(3)]
    for copy in copies:
        copy.start()
    for copy in copies:
        copy.wait()


def solution(mesh):
    constants, place = tables()

    def local(coarse, density, history, cell, offset, charge, width):
        coarse = jnp.transpose(coarse, (1, 0, 2))
        history = jnp.transpose(history, (1, 0, 2))
        offset = jnp.transpose(offset, (1, 2, 3, 0))
        inputs = (cell, offset, charge, width, coarse, density, history)
        inputs = (*inputs, jnp.asarray(constants))
        vmem = pl.BlockSpec(memory_space=pltpu.VMEM)
        dma = pltpu.SemaphoreType.DMA
        tile = (NY, 8, 128)
        residual, potential, sums = pl.pallas_call(
            functools.partial(kernel, place),
            out_shape=(
                pltpu.VMEM((FZ, FY * NF), F32),
                pltpu.VMEM((FZ, FY * NF), F32),
                pltpu.VMEM((HIST + 1,), F32),
            ),
            in_specs=[pl.BlockSpec(memory_space=pltpu.HBM)] * len(inputs),
            out_specs=(vmem, vmem, vmem),
            scratch_shapes=[
                *(pltpu.VMEM(i.shape, i.dtype) for i in inputs),
                pltpu.VMEM((18, 8, NC), F32),
                pltpu.VMEM((9, 8, 128), F32),
                *[pltpu.VMEM((128, 128), F32)] * 4,
                *[pltpu.VMEM((648, 128), F32)] * 2,
                *[pltpu.VMEM(tile, F32)] * 2,
                pltpu.VMEM((256, 128), F32),
                *[pltpu.VMEM((264, 128), F32)] * 3,
                *[pltpu.VMEM(tile, F32)] * 2,
                *[pltpu.VMEM((NY, EARLY, 8, 128), F32)] * 2,
                *[pltpu.VMEM((NY, HIST - EARLY, 8, 128), F32)] * 2,
                pltpu.VMEM((NF, 128), F32),
                pltpu.VMEM((NY, 1, 128), F32),
                pltpu.VMEM((NZ, 1, 128), F32),
                dma((8,)), dma, dma, dma, dma((3,)),
                *[dma] * 16,
                *[pltpu.SemaphoreType.REGULAR] * 3,
            ],
            compiler_params=pltpu.CompilerParams(collective_id=0, has_side_effects=True),
        )(*inputs)
        results = tuple(pltpu.with_memory_space_constraint(r, pltpu.VMEM) for r in (residual, potential, sums))
        hbm = pl.BlockSpec(memory_space=pltpu.HBM)
        return pl.pallas_call(
            write_out,
            out_shape=tuple(jax.ShapeDtypeStruct(r.shape, F32) for r in results),
            in_specs=[vmem] * 3,
            out_specs=(hbm,) * 3,
            scratch_shapes=[dma((3,))],
        )(*results)

    in_specs = (
        P(None, "gy", None),
        P("gz", "gy"),
        P(None, "gz", "gy"),
        P("gz", "gy", None),
        P(None, "gz", "gy", None),
        P("gz", "gy", None),
        P("gz", "gy", None),
    )
    out_specs = (P("gz", "gy"), P("gz", "gy"), P())
    return jax.shard_map(local, mesh=mesh, in_specs=in_specs, out_specs=out_specs, check_vma=False)
```

```python
import functools

import jax
import jax.numpy as jnp
import numpy as np
from jax import lax
from jax.experimental import pallas as pl
from jax.experimental.pallas import tpu as pltpu
from jax.sharding import PartitionSpec as P

MESH = pl.DeviceIdType.MESH
NC = 96
NF = 192
HIST = 8
EARLY = 3
RC = 4
FZ = 6
FY = 12
NZ = 32
NY = 16
KX = NF // NY
KY = NF // NZ
STENCIL = ((-1, -1.0 / 16.0), (0, 9.0 / 16.0), (1, 9.0 / 16.0), (2, -1.0 / 16.0))
F32 = jnp.float32
BF16 = jnp.bfloat16


def two(table):
    high = np.asarray(table, np.float32).astype(jnp.bfloat16)
    low = (table - high.astype(np.float64)).astype(np.float32).astype(jnp.bfloat16)
    return high, low


def hartley():
    n = np.arange(NF)
    angle = 2.0 * np.pi / NF * (n[:, None] * n[None, :] % NF)
    return (np.cos(angle) + np.sin(angle)) / np.sqrt(NF)


def tables():
    h = hartley()
    rep = np.zeros((256, NY, 128))
    for j in range(NY):
        for g in range(9):
            rep[:NF, j, g * KX : (g + 1) * KX] = h[:, j * KX : (j + 1) * KX]
    rep = rep.reshape(256, NY * 128)
    by_y = h.reshape(NZ, KY, NY, FY)
    by_y = np.stack([by_y[:, :4], by_y[:, [4, 4, 5, 5]]])
    fy = np.stack([by_y[..., :8], by_y[..., [8, 9, 10, 11, 8, 9, 10, 11]]], axis=3)
    fy = fy.reshape(256, 256)
    fz = h.reshape(NF, NZ, FZ).transpose(0, 2, 1).reshape(NF, NF)
    ix = np.zeros((256, NC))
    for i in range(NC):
        ix[2 * i, i] = 1.0
        for offset, value in STENCIL:
            ix[2 * i + 1, (i + offset) % NC] += value
    wy = np.zeros((FY, FY // 2 + 3))
    for i in range(FY // 2):
        wy[2 * i, i + 1] = 1.0
        for offset, value in STENCIL:
            wy[2 * i + 1, i + 1 + offset] += value
    place = [(1, 5)] + [(0, r) for r in range(6)] + [(2, 0), (2, 1)]
    spread_y = np.zeros((72, 3, 6, 8))
    for z in range(FZ):
        for y in range(FY):
            row = 8 * z + y if y < 8 else 48 + 8 * (z % 3) + 4 * (z // 3) + y - 8
            for r, (block, coarse_y) in enumerate(place):
                spread_y[row, block, coarse_y, z] = wy[y, r]
    exact = [t.astype(np.float32).astype(jnp.bfloat16) for t in (ix.T, spread_y.reshape(72, 144))]
    pieces = {"ix": exact[0], "spread_y": exact[1]}
    for name, table in (("fy", fy), ("gy", fy.T), ("fz", fz), ("gz", fz.T)):
        pieces[name + "_h"], pieces[name + "_l"] = two(table)
    by_span = rep.reshape(256, NY // 2, 256).transpose(1, 0, 2).reshape(-1, 256)
    pieces["rep_h"], pieces["rep_l"] = two(by_span)
    place, stack, row = {}, [], 0
    for name, piece in pieces.items():
        rows, columns = piece.shape
        place[name] = (row, rows, columns)
        stack.append(np.pad(piece, ((0, -rows % 16), (0, 256 - columns))))
        row += rows + -rows % 16
    return np.concatenate(stack, axis=0), place


def split2(value):
    high = value.astype(BF16)
    return high, (value - high.astype(F32)).astype(BF16)


def split3(value):
    high = value.astype(BF16)
    rest = value - high.astype(F32)
    middle = rest.astype(BF16)
    return high, middle, (rest - middle.astype(F32)).astype(BF16)


def dot(a, b):
    return jnp.dot(a, b, preferred_element_type=F32)


def dot_nt(a, b):
    return lax.dot_general(a, b, (((1,), (1,)), ((), ())), preferred_element_type=F32)


def dot3(a, b, product=dot):
    return product(a[0], b[0]) + product(a[1], b[0]) + product(a[0], b[1])


def dot_data(table, value):
    high, low = split2(value)
    width = value.shape[1]
    both = dot(table[0], jnp.concatenate([high, low], axis=1))
    return both[:, :width] + (both[:, width:] + dot(table[1], high))


def wrap(index, count):
    return jnp.where(index >= count, index - count, index)


def each_partner(me, count, act):
    act(wrap(me + count // 2, count))

    def body(t, _):
        act(wrap(me + count // 2 - t, count))
        act(wrap(me + count // 2 + t, count))
        return 0

    lax.fori_loop(1, count // 2, body, 0, unroll=True)


def kernel(
    place, cell_in, offset_in, charge_in, width_in, coarse_in, density_in, history_in, tables_in, *refs
):
    residual_out, potential_out, sums_out = refs[:3]
    (
        cell, offset, charge, width, coarse, density, history, all_tables,
        planes, atoms, field_0, field_1, out_0, out_1, hist_0, hist_1,
        send1, recv1, send2, recv2, send4, recv4, send5, recv5, send_g, recv_g, send_h, recv_h,
        weight, row_a, row_b,
        load_sem, halo_send, halo_recv, atom_send, atom_recv,
        s1, r1, s2, r2, s4, r4, s5, r5, sg, rg, sh, rh, sa, ra, sb, rb, ring_z_ready, ring_y_ready, plane_ready,
    ) = refs[3:]
    gz = lax.axis_index("gz")
    gy = lax.axis_index("gy")

    def zy(dz, dy):
        return (wrap(wrap(gz + dz + NZ, NZ), NZ) if dz else gz, wrap(wrap(gy + dy + NY, NY), NY) if dy else gy)

    barrier = pltpu.get_barrier_semaphore()

    def greet(semaphore, z, y):
        pl.semaphore_signal(semaphore, inc=1, device_id=(z, y), device_id_type=MESH)

    column = lax.rem(gz, 4)
    ring_x = [gz - column + lax.rem(column + k, 4) for k in (2, 1, 3)]
    other_core = gy + 1 - 2 * lax.rem(gy, 2)
    greeted = [zy(dz, dy) for dz in (-1, 1) for dy in (-1, 1)]
    greeted += [zy(dz, 0) for dz in (-8, 8)] + [(j, gy) for j in ring_x]
    greeted += [(gz, wrap(wrap(core + dy + NY, NY), NY)) for dy in (-4, 4, -2, 2) for core in (gy, other_core)]
    greeted += [zy(dz, 0) for dz in (-4, 4, -1, 1)] + [(gz, other_core)]
    for z, y in greeted:
        greet(barrier, z, y)

    sources = (
        cell_in, offset_in, charge_in, width_in, coarse_in, density_in, tables_in, history_in,
    )
    targets = (cell, offset, charge, width, coarse, density, all_tables, history)
    loads = {}
    for k, (source, target) in enumerate(zip(sources, targets)):
        loads[k] = pltpu.make_async_copy(source, target, load_sem.at[k])
        loads[k].start()

    def table(name):
        row, rows, columns = place[name]
        return all_tables[row : row + rows, :columns]

    def spans(p):
        return tuple(
            all_tables[place[name][0] + 256 * p : place[name][0] + 256 * p + 256, :]
            for name in ("rep_h", "rep_l")
        )

    row8 = lax.broadcasted_iota(jnp.int32, (8, 128), 0)
    lane8 = lax.broadcasted_iota(jnp.int32, (8, 128), 1)
    group = jnp.zeros_like(lane8)
    for c in range(1, 11):
        group = group + (lane8 >= c * KX).astype(jnp.int32)

    def square(counter):
        wave = jnp.where(counter < NF // 2, counter, counter - NF)
        return wave * wave

    wave_yx = (square(gz * KY + group) + square(gy * KX + lane8 - KX * group))[0:1]
    used = (lane8 < KY * KX)[0:1]
    squares = square(lax.broadcasted_iota(jnp.int32, (NF, 128), 0)) + wave_yx
    scaled = (2.0 * np.pi / NF) ** 2 * jnp.maximum(squares, 1).astype(F32)
    weight[...] = jnp.where((squares > 0) & used, 4.0 * np.pi / scaled, 0.0)

    for k in range(4):
        loads[k].wait()

    def whole_tile(value):
        return jnp.broadcast_to(value, (8, 128))

    site = whole_tile(cell[0].astype(F32))
    site_z = jnp.zeros((8, 128), F32)
    for k in range(1, FZ):
        site_z = site_z + (site >= float(k * FY * NF)).astype(F32)
    site = site - site_z * float(FY * NF)
    site_y = jnp.zeros((8, 128), F32)
    for k in range(1, FY):
        site_y = site_y + (site >= float(k * NF)).astype(F32)
    site_x = site - site_y * float(NF)
    own = whole_tile(width[0])
    offsets = offset[0, 0]
    for k, value in enumerate(
        (site_z, site_y, site_x, *(whole_tile(offsets[:, i : i + 1]) for i in range(3)), whole_tile(charge[0]))
    ):
        own = jnp.where(row8 == k, value, own)
    atoms[4] = own

    pl.semaphore_wait(barrier, len(greeted))

    neighbours = {}
    for dz in (-1, 1, 0):
        for dy in (-1, 1, 0):
            if (dz, dy) != (0, 0):
                slot = (1 - dz) * 3 + 1 - dy
                neighbours[slot] = pltpu.make_async_remote_copy(
                    atoms.at[4], atoms.at[slot], atom_send, atom_recv.at[2 * abs(dz) + abs(dy) - 1],
                    device_id=zy(dz, dy), device_id_type=MESH,
                )
    for copy in neighbours.values():
        copy.start()
    for dy in (-4, 4):
        greet(ring_z_ready, *zy(0, dy))
    for dz in (-8, 8):
        greet(ring_y_ready, *zy(dz, 0))

    plane_of = lax.broadcasted_iota(jnp.int32, (8, NC), 1)
    fine_of = lax.broadcasted_iota(jnp.int32, (8, NC), 0)
    away = plane_of - gz * (FZ // 2) - fine_of // 2
    away = jnp.where(away < 0, away + NC, away)
    odd = jnp.zeros((8, NC), F32)
    for shift, value in STENCIL:
        odd = jnp.where(away == shift % NC, value, odd)
    even = jnp.where(away == 0, 1.0, 0.0)
    along_z = jnp.where(fine_of % 2 == 1, odd, even)
    along_z = jnp.where(fine_of < FZ, along_z, 0.0).astype(BF16)
    loads[4].wait()
    for k in range(6):
        parts = split3(coarse[k])
        planes[k] = dot(along_z, parts[0]) + dot(along_z, parts[1]) + dot(along_z, parts[2])

    own_planes = planes.at[pl.ds(0, 6)]
    halos = [
        pltpu.make_async_remote_copy(
            own_planes, planes.at[pl.ds(6 * k, 6)], halo_send, halo_recv,
            device_id=zy(0, dy), device_id_type=MESH,
        )
        for k, dy in ((1, 1), (2, -1))
    ]
    for copy in halos:
        copy.start()

    lane128 = lax.broadcasted_iota(jnp.int32, (FZ, 128), 1)
    loads[5].wait()

    def put(y, low, high):
        if y < 8:
            field_0[pl.ds(y, FZ, stride=8), :] = low
            field_1[pl.ds(y, FZ, stride=8), :] = high
        else:
            for half in range(2):
                rows = pl.ds(40 + y + 4 * half, 3, stride=8)
                field_0[rows, :] = low[3 * half : 3 * half + 3]
                field_1[rows, :] = high[3 * half : 3 * half + 3]

    for pair in range(FY // 2):
        a, b, c = (density[:, 384 * pair + 128 * k : 384 * pair + 128 * k + 128] for k in range(3))
        rolled_b = pltpu.roll(b, 64, 1)
        rolled_c = pltpu.roll(c, 64, 1)
        put(2 * pair, a, b)
        put(2 * pair + 1, jnp.where(lane128 < 64, rolled_b, rolled_c), rolled_c)

    x = lax.broadcasted_iota(jnp.int32, (1, 256), 1).astype(F32)
    y_low = row8.astype(F32)
    y_high = jnp.where(row8 < 4, row8 + 8, row8 + 4).astype(F32)
    z = row8.astype(F32)

    def double(value):
        return jnp.concatenate([value, value], axis=1)

    upper = double(row8) < 4

    def charge_of(k):
        tile = atoms[k]
        dz, dy = k // 3 - 1, k % 3 - 1
        exponent = tile[7:8]
        wide = double(tile)
        from_z = (z - float(FZ * dz) - tile[0:1]) - tile[3:4]
        from_low = (y_low - float(FY * dy) - tile[1:2]) - tile[4:5]
        from_high = (y_high - float(FY * dy) - tile[1:2]) - tile[4:5]
        from_x = x - wide[2:3]
        from_x = jnp.where(from_x >= NF / 2, from_x - NF, from_x)
        from_x = jnp.where(from_x < -NF / 2, from_x + NF, from_x)
        from_x = from_x - wide[5:6]
        exp_z = double(jnp.exp(-exponent * (from_z * from_z)))
        exp_x = jnp.exp(-wide[7:8] * (from_x * from_x))
        low = double(jnp.exp(-exponent * (from_low * from_low))) * exp_x
        high = double(jnp.exp(-exponent * (from_high * from_high))) * exp_x
        floor = jnp.exp(-wide[7:8] * float(RC * RC))
        ratio = wide[7:8] / np.pi
        factor = wide[6:7] * (ratio * jnp.sqrt(ratio))
        powers = [low * exp_z[c : c + 1] for c in range(FZ)]
        powers += [high * jnp.where(upper, exp_z[c : c + 1], exp_z[c + 3 : c + 4]) for c in range(3)]
        return [factor * jnp.maximum(power - floor, 0.0) for power in powers]

    total = charge_of(4)

    group256 = double(group)

    def along_x_forward(values, store):
        count = values.shape[0]
        high, low = split2(values)
        both = jnp.concatenate([high, low], axis=0)
        for p in range(NY // 2):
            rep_h, rep_l = spans(p)
            out = dot(both, rep_h)
            out = out[:count] + (out[count:] + dot(high, rep_l))
            for i in range(count // 72):
                chosen = out[72 * i : 72 * i + 8]
                for g in range(1, 9):
                    chosen = jnp.where(group256 >= g, out[72 * i + 8 * g : 72 * i + 8 * g + 8], chosen)
                store(2 * p, i, chosen[:, :128])
                store(2 * p + 1, i, chosen[:, 128:])

    def history_along_x(first, count, send):
        def store(j, i, value):
            send[j, i] = value

        rows = slice(72 * first, 72 * (first + count))
        along_x_forward(jnp.concatenate([hist_0[rows, :], hist_1[rows, :]], axis=1), store)

    loads[7].wait()
    lane_h = lax.broadcasted_iota(jnp.int32, (HIST, 128), 1)
    for c in range(FZ):
        for pair in range(FY // 2):
            a, b, d = (history[c, :, 384 * pair + 128 * k : 384 * pair + 128 * k + 128] for k in range(3))
            rolled_b = pltpu.roll(b, 64, 1)
            rolled_d = pltpu.roll(d, 64, 1)
            for y, low, high in (
                (2 * pair, a, jnp.where(lane_h < 64, b, 0.0)),
                (2 * pair + 1, jnp.where(lane_h < 64, rolled_b, rolled_d), jnp.where(lane_h < 64, rolled_d, 0.0)),
            ):
                row = 8 * c + y if y < 8 else 48 + 8 * (c % 3) + 4 * (c // 3) + y - 8
                hist_0[pl.ds(row, HIST, stride=72), :] = low
                hist_1[pl.ds(row, HIST, stride=72), :] = high
    loads[6].wait()
    history_along_x(0, EARLY, send_g)

    whole = planes.at[pl.ds(0, 12)]
    pltpu.make_async_copy(whole, whole, halo_recv).wait()
    parts = split3(planes[...].reshape(144, NC))
    weights = table("ix")
    along_x = dot(parts[0], weights) + dot(parts[1], weights) + dot(parts[2], weights)
    parts = split3(along_x)
    weights = table("spread_y")
    smooth = dot(weights, parts[0]) + dot(weights, parts[1]) + dot(weights, parts[2])

    for kind, slots in ((0, (3, 5)), (1, (1, 7)), (2, (0, 2, 6, 8))):
        whole = atoms.at[pl.ds(0, len(slots))]
        pltpu.make_async_copy(whole, whole, atom_recv.at[kind]).wait()
        for k in slots:
            total = [a + b for a, b in zip(total, charge_of(k))]

    inside = lax.broadcasted_iota(jnp.int32, (8, 256), 1) < NF
    blocks = []
    for g in range(9):
        rows = slice(8 * g, 8 * g + 8)
        given = jnp.concatenate([field_0[rows, :], field_1[rows, :]], axis=1)
        value = jnp.where(inside, smooth[rows] + total[g] - given, 0.0)
        blocks.append(value)
        field_0[rows, :] = value[:, :128]
        field_1[rows, :] = value[:, 128:]

    def exchange_y(send, recv, ssem, rsem):
        def act(j):
            pltpu.make_async_remote_copy(
                send.at[j], recv.at[gy], ssem, rsem, device_id=(gz, j), device_id_type=MESH
            ).start()

        each_partner(gy, NY, act)
        recv[gy] = send[gy]
        whole = recv.at[pl.ds(0, NY - 1)]
        return pltpu.make_async_copy(whole, whole, rsem), pltpu.make_async_copy(whole, whole, ssem)

    def exchange_z(send, recv, ssem, rsem):
        mine = pl.ds(pl.multiple_of(gz * 4, 4), 4)

        def act(j):
            pltpu.make_async_remote_copy(
                send.at[pl.ds(pl.multiple_of(j * 4, 4), 4)], recv.at[mine],
                ssem, rsem, device_id=(j, gy), device_id_type=MESH,
            ).start()

        each_partner(gz, NZ, act)
        recv[mine, :] = send[mine, :]
        whole = recv.at[pl.ds(0, 4 * (NZ - 1))]
        return pltpu.make_async_copy(whole, whole, rsem), pltpu.make_async_copy(whole, whole, ssem)

    pl.semaphore_wait(ring_z_ready, 2)
    high, low = split2(jnp.concatenate(blocks, axis=0))
    both = jnp.concatenate([high, low], axis=0)
    chip = gy // 2
    for part in ((4, 3, 5), (2, 6, 1, 7, 0)):
        done = []
        for away in part:
            p = wrap(chip + away, NY // 2)
            rows = [
                all_tables[pl.ds(pl.multiple_of(place[name][0] + 256 * p, 16), 256), :]
                for name in ("rep_h", "rep_l")
            ]
            out = dot(both, rows[0])
            out = out[:72] + (out[72:] + dot(high, rows[1]))
            chosen = out[0:8]
            for g in range(1, 9):
                chosen = jnp.where(group256 >= g, out[8 * g : 8 * g + 8], chosen)
            done.append((away, p, chosen))
        for away, p, chosen in done:
            send1[2 * p] = chosen[:, :128]
            send1[2 * p + 1] = chosen[:, 128:]
        for away, p, _ in done:
            for j in (2 * p, 2 * p + 1) if away else (other_core,):
                pltpu.make_async_remote_copy(
                    send1.at[j], recv1.at[gy], s1, r1, device_id=(gz, j), device_id_type=MESH
                ).start()
    recv1[gy] = send1[gy]
    whole = recv1.at[pl.ds(0, NY - 1)]
    arrived = pltpu.make_async_copy(whole, whole, r1)
    sent1 = pltpu.make_async_copy(whole, whole, s1)
    arrived_g, sent_g = exchange_y(send_g, recv_g, sg, rg)
    pl.semaphore_wait(ring_y_ready, 2)
    for j in ring_x:
        greet(plane_ready, j, gy)
    history_along_x(EARLY, HIST - EARLY, send_h)
    arrived_h, sent_h = exchange_y(send_h, recv_h, sh, rh)

    groups128 = jnp.concatenate([group] * NY, axis=0)
    rows128 = jnp.concatenate([row8] * NY, axis=0)
    from_upper = (groups128 < 3) & (rows128 < 4)
    from_lower = (groups128 >= 3) & (groups128 < 6) & (rows128 >= 4)
    arrived.wait()
    packed = recv1[...].reshape(128, 128)
    moved = jnp.where(
        from_upper, pltpu.roll(packed, 128 - 72, 1), jnp.where(from_lower, pltpu.roll(packed, 128 - 36, 1), 0.0)
    )
    even_rows = rows128 % 2 == 0
    out = dot_data((table("fy_h"), table("fy_l")), jnp.concatenate([packed, moved], axis=0))
    high = out[128:]
    send2[0:128, :] = jnp.where(
        groups128 < 6, out[:128], jnp.where(even_rows, pltpu.roll(high, 72, 1), pltpu.roll(high, 36, 1))
    )
    pl.semaphore_wait(plane_ready, 3)
    arrived, sent2 = exchange_z(send2, recv2, s2, r2)

    def give(out, first, second):
        for pair in range(FY // 2):
            if pair < 4:
                places = ((0, FZ, 2 * pair),)
            else:
                places = ((0, 3, 40 + 2 * pair), (3, 3, 44 + 2 * pair))
            for top, count, row in places:
                low_lanes = lax.broadcasted_iota(jnp.int32, (count, 128), 1) < 64
                a = first[pl.ds(row, count, stride=8), :]
                b = second[pl.ds(row, count, stride=8), :]
                c = pltpu.roll(first[pl.ds(row + 1, count, stride=8), :], 64, 1)
                d = pltpu.roll(second[pl.ds(row + 1, count, stride=8), :], 64, 1)
                tiles = (a, jnp.where(low_lanes, b, c), jnp.where(low_lanes, c, d))
                for k, tile in enumerate(tiles):
                    out[top : top + count, 384 * pair + 128 * k : 384 * pair + 128 * k + 128] = tile

    give(residual_out, field_0, field_1)
    arrived.wait()

    group1 = group[0:1]

    def swapped(pieces, position):
        result = None
        for b in range(6):
            shift = (KX * (b - position)) % 128
            moved = pltpu.roll(pieces[b], shift, 1) if shift else pieces[b]
            result = moved if result is None else jnp.where(group1 >= b, moved, result)
        return result

    packed_rows = [recv2[pl.ds(r, NZ, stride=4), :] for r in range(4)]
    pieces = packed_rows + [
        jnp.where(group1 < 3, pltpu.roll(packed_rows[r], 128 - 72, 1), pltpu.roll(packed_rows[r + 1], 128 - 36, 1))
        for r in (0, 2)
    ]
    stacked = jnp.concatenate([swapped(pieces, a) for a in range(FZ)], axis=0)
    spectrum = dot_data((table("fz_h"), table("fz_l")), (stacked)) * weight[...]
    back = dot_data((table("gz_h"), table("gz_l")), (spectrum))
    pieces = [back[NZ * a : NZ * a + NZ] for a in range(FZ)]
    pieces = [swapped(pieces, b) for b in range(KY)]
    for r in range(4):
        beside = pltpu.roll(pieces[4 + r // 2], 36 if r % 2 else 72, 1)
        send4[pl.ds(r, NZ, stride=4), :] = jnp.where(group1 < 6, pieces[r], beside)
    arrived, sent4 = exchange_z(send4, recv4, s4, r4)
    arrived.wait()

    packed = recv4[0:128, :]
    moved = jnp.where(
        even_rows & (groups128 < 3), pltpu.roll(packed, 128 - 72, 1),
        jnp.where((rows128 % 2 == 1) & (groups128 >= 3) & (groups128 < 6), pltpu.roll(packed, 128 - 36, 1), 0.0),
    )
    out = dot_data((table("gy_h"), table("gy_l")), jnp.concatenate([packed, moved], axis=0))
    low, high = out[:128], out[128:]
    packed = jnp.where(
        groups128 < 6, low, jnp.where(rows128 < 4, pltpu.roll(high, 72, 1), pltpu.roll(high, 36, 1))
    )
    arrived_g.wait()
    arrived_h.wait()
    terms = [jnp.zeros((8, 128), F32) for _ in range(HIST + 1)]
    for j in range(NY):
        tile = jnp.where(group < 9, packed[8 * j : 8 * j + 8], 0.0)
        for i in range(EARLY):
            terms[i] = terms[i] + recv_g[j, i] * tile
        for i in range(EARLY, HIST):
            terms[i] = terms[i] + recv_h[j, i - EARLY] * tile
        terms[HIST] = terms[HIST] + recv1[j] * tile
    rows = jnp.concatenate(
        [jnp.sum(t, axis=0, keepdims=True) for t in terms] + [jnp.zeros((7, 128), F32)], axis=0
    ) * (1.0 / float(NF) ** 3)
    column = jnp.sum(rows, axis=1, keepdims=True)
    lane_of = lax.broadcasted_iota(jnp.int32, (16, 128), 1)
    row_of = lax.broadcasted_iota(jnp.int32, (16, 128), 0)
    line = jnp.sum(jnp.where(lane_of == row_of, column, 0.0), axis=0, keepdims=True)

    row_b[gz] = line

    def act_b(j):
        pltpu.make_async_remote_copy(
            row_b.at[gz], row_b.at[gz], sb, rb, device_id=(j, gy), device_id_type=MESH
        ).start()

    each_partner(gz, NZ, act_b)
    for j in range(NY):
        send5[j] = packed[8 * j : 8 * j + 8]
    arrived, sent5 = exchange_y(send5, recv5, s5, r5)
    whole_b = row_b.at[pl.ds(0, NZ - 1)]
    pltpu.make_async_copy(whole_b, whole_b, rb).wait()
    row_a[gy] = jnp.sum(row_b[...], axis=0)

    def act_a(j):
        pltpu.make_async_remote_copy(
            row_a.at[gy], row_a.at[gy], sa, ra, device_id=(gz, j), device_id_type=MESH
        ).start()

    each_partner(gy, NY, act_a)

    arrived.wait()
    potential = jnp.zeros((72, 256), F32)
    for p in range(NY // 2):
        pair = split2(jnp.concatenate([recv5[2 * p], recv5[2 * p + 1]], axis=1))
        masked = [
            jnp.concatenate([jnp.where(group256 == g, part.astype(F32), 0.0) for g in range(9)], axis=0).astype(BF16)
            for part in pair
        ]
        potential = potential + dot3(masked, spans(p), dot_nt)
    out_0[0:72, :] = potential[:, :128]
    out_1[0:72, :] = potential[:, 128:]
    give(potential_out, out_0, out_1)

    whole = atoms.at[pl.ds(0, 8)]
    pltpu.make_async_copy(whole, whole, atom_send).wait()
    whole = planes.at[pl.ds(0, 12)]
    pltpu.make_async_copy(whole, whole, halo_send).wait()
    for copy in (sent1, sent2, sent_g, sent_h, sent4, sent5):
        copy.wait()
    pltpu.make_async_copy(whole_b, whole_b, sb).wait()
    whole_a = row_a.at[pl.ds(0, NY - 1)]
    pltpu.make_async_copy(whole_a, whole_a, sa).wait()
    pltpu.make_async_copy(whole_a, whole_a, ra).wait()
    sums_out[...] = jnp.sum(row_a[...], axis=0)[0, : HIST + 1]


def write_out(*refs):
    copies = [pltpu.make_async_copy(refs[k], refs[3 + k], refs[6].at[k]) for k in range(3)]
    for copy in copies:
        copy.start()
    for copy in copies:
        copy.wait()


def solution(mesh):
    constants, place = tables()

    def local(coarse, density, history, cell, offset, charge, width):
        coarse = jnp.transpose(coarse, (1, 0, 2))
        history = jnp.transpose(history, (1, 0, 2))
        offset = jnp.transpose(offset, (1, 2, 3, 0))
        inputs = (cell, offset, charge, width, coarse, density, history)
        inputs = (*inputs, jnp.asarray(constants))
        vmem = pl.BlockSpec(memory_space=pltpu.VMEM)
        dma = pltpu.SemaphoreType.DMA
        tile = (NY, 8, 128)
        residual, potential, sums = pl.pallas_call(
            functools.partial(kernel, place),
            out_shape=(
                pltpu.VMEM((FZ, FY * NF), F32),
                pltpu.VMEM((FZ, FY * NF), F32),
                pltpu.VMEM((HIST + 1,), F32),
            ),
            in_specs=[pl.BlockSpec(memory_space=pltpu.HBM)] * len(inputs),
            out_specs=(vmem, vmem, vmem),
            scratch_shapes=[
                *(pltpu.VMEM(i.shape, i.dtype) for i in inputs),
                pltpu.VMEM((18, 8, NC), F32),
                pltpu.VMEM((9, 8, 128), F32),
                *[pltpu.VMEM((128, 128), F32)] * 4,
                *[pltpu.VMEM((648, 128), F32)] * 2,
                *[pltpu.VMEM(tile, F32)] * 2,
                *[pltpu.VMEM((136, 128), F32)] * 4,
                *[pltpu.VMEM(tile, F32)] * 2,
                *[pltpu.VMEM((NY, EARLY, 8, 128), F32)] * 2,
                *[pltpu.VMEM((NY, HIST - EARLY, 8, 128), F32)] * 2,
                pltpu.VMEM((NF, 128), F32),
                pltpu.VMEM((NY, 1, 128), F32),
                pltpu.VMEM((NZ, 1, 128), F32),
                dma((8,)), dma, dma, dma, dma((3,)),
                *[dma] * 16,
                *[pltpu.SemaphoreType.REGULAR] * 3,
            ],
            compiler_params=pltpu.CompilerParams(collective_id=0, has_side_effects=True),
        )(*inputs)
        results = tuple(pltpu.with_memory_space_constraint(r, pltpu.VMEM) for r in (residual, potential, sums))
        hbm = pl.BlockSpec(memory_space=pltpu.HBM)
        return pl.pallas_call(
            write_out,
            out_shape=tuple(jax.ShapeDtypeStruct(r.shape, F32) for r in results),
            in_specs=[vmem] * 3,
            out_specs=(hbm,) * 3,
            scratch_shapes=[dma((3,))],
        )(*results)

    in_specs = (
        P(None, "gy", None),
        P("gz", "gy"),
        P(None, "gz", "gy"),
        P("gz", "gy", None),
        P(None, "gz", "gy", None),
        P("gz", "gy", None),
        P("gz", "gy", None),
    )
    out_specs = (P("gz", "gy"), P("gz", "gy"), P())
    return jax.shard_map(local, mesh=mesh, in_specs=in_specs, out_specs=out_specs, check_vma=False)
```

```python
import functools

import jax
import jax.numpy as jnp
import numpy as np
from jax import lax
from jax.experimental import pallas as pl
from jax.experimental.pallas import tpu as pltpu
from jax.sharding import PartitionSpec as P

MESH = pl.DeviceIdType.MESH
NC = 96
NF = 192
HIST = 8
EARLY = 3
RC = 4
FZ = 6
FY = 12
NZ = 32
NY = 16
KX = NF // NY
KY = NF // NZ
STENCIL = ((-1, -1.0 / 16.0), (0, 9.0 / 16.0), (1, 9.0 / 16.0), (2, -1.0 / 16.0))
F32 = jnp.float32
BF16 = jnp.bfloat16


def two(table):
    high = np.asarray(table, np.float32).astype(jnp.bfloat16)
    low = (table - high.astype(np.float64)).astype(np.float32).astype(jnp.bfloat16)
    return high, low


def hartley():
    n = np.arange(NF)
    angle = 2.0 * np.pi / NF * (n[:, None] * n[None, :] % NF)
    return (np.cos(angle) + np.sin(angle)) / np.sqrt(NF)


def tables():
    h = hartley()
    rep = np.zeros((256, NY, 128))
    for j in range(NY):
        for g in range(9):
            rep[:NF, j, g * KX : (g + 1) * KX] = h[:, j * KX : (j + 1) * KX]
    rep = rep.reshape(256, NY * 128)
    by_y = h.reshape(NZ, KY, NY, FY)
    by_y = np.stack([by_y[:, :4], by_y[:, [4, 4, 5, 5]]])
    fy = np.stack([by_y[..., :8], by_y[..., [8, 9, 10, 11, 8, 9, 10, 11]]], axis=3)
    fy = fy.reshape(256, 256)
    fz = h.reshape(NF, NZ, FZ).transpose(0, 2, 1).reshape(NF, NF)
    ix = np.zeros((256, NC))
    for i in range(NC):
        ix[2 * i, i] = 1.0
        for offset, value in STENCIL:
            ix[2 * i + 1, (i + offset) % NC] += value
    wy = np.zeros((FY, FY // 2 + 3))
    for i in range(FY // 2):
        wy[2 * i, i + 1] = 1.0
        for offset, value in STENCIL:
            wy[2 * i + 1, i + 1 + offset] += value
    place = [(1, 5)] + [(0, r) for r in range(6)] + [(2, 0), (2, 1)]
    spread_y = np.zeros((72, 3, 6, 8))
    for z in range(FZ):
        for y in range(FY):
            row = 8 * z + y if y < 8 else 48 + 8 * (z % 3) + 4 * (z // 3) + y - 8
            for r, (block, coarse_y) in enumerate(place):
                spread_y[row, block, coarse_y, z] = wy[y, r]
    exact = [t.astype(np.float32).astype(jnp.bfloat16) for t in (ix.T, spread_y.reshape(72, 144))]
    pieces = {"ix": exact[0], "spread_y": exact[1]}
    for name, table in (("fy", fy), ("gy", fy.T), ("fz", fz), ("gz", fz.T)):
        pieces[name + "_h"], pieces[name + "_l"] = two(table)
    by_span = rep.reshape(256, NY // 2, 256).transpose(1, 0, 2).reshape(-1, 256)
    pieces["rep_h"], pieces["rep_l"] = two(by_span)
    place, stack, row = {}, [], 0
    for name, piece in pieces.items():
        rows, columns = piece.shape
        place[name] = (row, rows, columns)
        stack.append(np.pad(piece, ((0, -rows % 16), (0, 256 - columns))))
        row += rows + -rows % 16
    return np.concatenate(stack, axis=0), place


def split2(value):
    high = value.astype(BF16)
    return high, (value - high.astype(F32)).astype(BF16)


def split3(value):
    high = value.astype(BF16)
    rest = value - high.astype(F32)
    middle = rest.astype(BF16)
    return high, middle, (rest - middle.astype(F32)).astype(BF16)


def dot(a, b):
    return jnp.dot(a, b, preferred_element_type=F32)


def dot_nt(a, b):
    return lax.dot_general(a, b, (((1,), (1,)), ((), ())), preferred_element_type=F32)


def dot3(a, b, product=dot):
    return product(a[0], b[0]) + product(a[1], b[0]) + product(a[0], b[1])


def dot_data(table, value):
    high, low = split2(value)
    width = value.shape[1]
    both = dot(table[0], jnp.concatenate([high, low], axis=1))
    return both[:, :width] + (both[:, width:] + dot(table[1], high))


def wrap(index, count):
    return jnp.where(index >= count, index - count, index)


def each_partner(me, count, act):
    act(wrap(me + count // 2, count))

    def body(t, _):
        act(wrap(me + count // 2 - t, count))
        act(wrap(me + count // 2 + t, count))
        return 0

    lax.fori_loop(1, count // 2, body, 0, unroll=True)


def kernel(
    place, cell_in, offset_in, charge_in, width_in, coarse_in, density_in, history_in, tables_in, *refs
):
    residual_out, potential_out, sums_out = refs[:3]
    (
        cell, offset, charge, width, coarse, density, history, all_tables,
        planes, atoms, field_0, field_1, out_0, out_1, hist_0, hist_1,
        send1, recv1, send2, recv2, send4, recv4, send5, recv5, send_g, recv_g, send_h, recv_h,
        weight, row_a, row_b, hist_y,
        load_sem, halo_send, halo_recv, atom_send, atom_recv,
        s1, r1, s2, r2, s4, r4, s5, r5, sg, rg, sh, rh, sa, ra, sb, rb, ring_z_ready, ring_y_ready, plane_ready,
    ) = refs[3:]
    gz = lax.axis_index("gz")
    gy = lax.axis_index("gy")

    def zy(dz, dy):
        return (wrap(wrap(gz + dz + NZ, NZ), NZ) if dz else gz, wrap(wrap(gy + dy + NY, NY), NY) if dy else gy)

    barrier = pltpu.get_barrier_semaphore()

    def greet(semaphore, z, y):
        pl.semaphore_signal(semaphore, inc=1, device_id=(z, y), device_id_type=MESH)

    column = lax.rem(gz, 4)
    ring_x = [gz - column + lax.rem(column + k, 4) for k in (2, 1, 3)]
    other_core = gy + 1 - 2 * lax.rem(gy, 2)
    greeted = [zy(dz, dy) for dz in (-1, 1) for dy in (-1, 1)]
    greeted += [zy(dz, 0) for dz in (-8, 8)] + [(j, gy) for j in ring_x]
    greeted += [(gz, wrap(wrap(core + dy + NY, NY), NY)) for dy in (-4, 4, -2, 2) for core in (gy, other_core)]
    greeted += [zy(dz, 0) for dz in (-4, 4, -1, 1)] + [(gz, other_core)]
    for z, y in greeted:
        greet(barrier, z, y)

    sources = (
        cell_in, offset_in, charge_in, width_in, coarse_in, density_in, tables_in, history_in,
    )
    targets = (cell, offset, charge, width, coarse, density, all_tables, history)
    loads = {}
    for k, (source, target) in enumerate(zip(sources, targets)):
        loads[k] = pltpu.make_async_copy(source, target, load_sem.at[k])
        loads[k].start()

    def table(name):
        row, rows, columns = place[name]
        return all_tables[row : row + rows, :columns]

    def spans(p):
        return tuple(
            all_tables[place[name][0] + 256 * p : place[name][0] + 256 * p + 256, :]
            for name in ("rep_h", "rep_l")
        )

    row8 = lax.broadcasted_iota(jnp.int32, (8, 128), 0)
    lane8 = lax.broadcasted_iota(jnp.int32, (8, 128), 1)
    group = jnp.zeros_like(lane8)
    for c in range(1, 11):
        group = group + (lane8 >= c * KX).astype(jnp.int32)

    def square(counter):
        wave = jnp.where(counter < NF // 2, counter, counter - NF)
        return wave * wave

    wave_yx = (square(gz * KY + group) + square(gy * KX + lane8 - KX * group))[0:1]
    used = (lane8 < KY * KX)[0:1]
    squares = square(lax.broadcasted_iota(jnp.int32, (NF, 128), 0)) + wave_yx
    scaled = (2.0 * np.pi / NF) ** 2 * jnp.maximum(squares, 1).astype(F32)
    weight[...] = jnp.where((squares > 0) & used, 4.0 * np.pi / scaled, 0.0)

    for k in range(4):
        loads[k].wait()

    def whole_tile(value):
        return jnp.broadcast_to(value, (8, 128))

    site = whole_tile(cell[0].astype(F32))
    site_z = jnp.zeros((8, 128), F32)
    for k in range(1, FZ):
        site_z = site_z + (site >= float(k * FY * NF)).astype(F32)
    site = site - site_z * float(FY * NF)
    site_y = jnp.zeros((8, 128), F32)
    for k in range(1, FY):
        site_y = site_y + (site >= float(k * NF)).astype(F32)
    site_x = site - site_y * float(NF)
    own = whole_tile(width[0])
    offsets = offset[0, 0]
    for k, value in enumerate(
        (site_z, site_y, site_x, *(whole_tile(offsets[:, i : i + 1]) for i in range(3)), whole_tile(charge[0]))
    ):
        own = jnp.where(row8 == k, value, own)
    atoms[4] = own

    pl.semaphore_wait(barrier, len(greeted))

    neighbours = {}
    for dz in (-1, 1, 0):
        for dy in (-1, 1, 0):
            if (dz, dy) != (0, 0):
                slot = (1 - dz) * 3 + 1 - dy
                neighbours[slot] = pltpu.make_async_remote_copy(
                    atoms.at[4], atoms.at[slot], atom_send, atom_recv.at[2 * abs(dz) + abs(dy) - 1],
                    device_id=zy(dz, dy), device_id_type=MESH,
                )
    for copy in neighbours.values():
        copy.start()
    for dy in (-4, 4):
        greet(ring_z_ready, *zy(0, dy))
    for dz in (-8, 8):
        greet(ring_y_ready, *zy(dz, 0))

    plane_of = lax.broadcasted_iota(jnp.int32, (8, NC), 1)
    fine_of = lax.broadcasted_iota(jnp.int32, (8, NC), 0)
    away = plane_of - gz * (FZ // 2) - fine_of // 2
    away = jnp.where(away < 0, away + NC, away)
    odd = jnp.zeros((8, NC), F32)
    for shift, value in STENCIL:
        odd = jnp.where(away == shift % NC, value, odd)
    even = jnp.where(away == 0, 1.0, 0.0)
    along_z = jnp.where(fine_of % 2 == 1, odd, even)
    along_z = jnp.where(fine_of < FZ, along_z, 0.0).astype(BF16)
    loads[4].wait()
    for k in range(6):
        parts = split3(coarse[k])
        planes[k] = dot(along_z, parts[0]) + dot(along_z, parts[1]) + dot(along_z, parts[2])

    own_planes = planes.at[pl.ds(0, 6)]
    halos = [
        pltpu.make_async_remote_copy(
            own_planes, planes.at[pl.ds(6 * k, 6)], halo_send, halo_recv,
            device_id=zy(0, dy), device_id_type=MESH,
        )
        for k, dy in ((1, 1), (2, -1))
    ]
    for copy in halos:
        copy.start()

    lane128 = lax.broadcasted_iota(jnp.int32, (FZ, 128), 1)
    loads[5].wait()

    def put(y, low, high):
        if y < 8:
            field_0[pl.ds(y, FZ, stride=8), :] = low
            field_1[pl.ds(y, FZ, stride=8), :] = high
        else:
            for half in range(2):
                rows = pl.ds(40 + y + 4 * half, 3, stride=8)
                field_0[rows, :] = low[3 * half : 3 * half + 3]
                field_1[rows, :] = high[3 * half : 3 * half + 3]

    for pair in range(FY // 2):
        a, b, c = (density[:, 384 * pair + 128 * k : 384 * pair + 128 * k + 128] for k in range(3))
        rolled_b = pltpu.roll(b, 64, 1)
        rolled_c = pltpu.roll(c, 64, 1)
        put(2 * pair, a, b)
        put(2 * pair + 1, jnp.where(lane128 < 64, rolled_b, rolled_c), rolled_c)

    x = lax.broadcasted_iota(jnp.int32, (1, 256), 1).astype(F32)
    y_low = row8.astype(F32)
    y_high = jnp.where(row8 < 4, row8 + 8, row8 + 4).astype(F32)
    z = row8.astype(F32)

    def double(value):
        return jnp.concatenate([value, value], axis=1)

    upper = double(row8) < 4

    def charge_of(k):
        tile = atoms[k]
        dz, dy = k // 3 - 1, k % 3 - 1
        exponent = tile[7:8]
        wide = double(tile)
        from_z = (z - float(FZ * dz) - tile[0:1]) - tile[3:4]
        from_low = (y_low - float(FY * dy) - tile[1:2]) - tile[4:5]
        from_high = (y_high - float(FY * dy) - tile[1:2]) - tile[4:5]
        from_x = x - wide[2:3]
        from_x = jnp.where(from_x >= NF / 2, from_x - NF, from_x)
        from_x = jnp.where(from_x < -NF / 2, from_x + NF, from_x)
        from_x = from_x - wide[5:6]
        exp_z = double(jnp.exp(-exponent * (from_z * from_z)))
        exp_x = jnp.exp(-wide[7:8] * (from_x * from_x))
        low = double(jnp.exp(-exponent * (from_low * from_low))) * exp_x
        high = double(jnp.exp(-exponent * (from_high * from_high))) * exp_x
        floor = jnp.exp(-wide[7:8] * float(RC * RC))
        ratio = wide[7:8] / np.pi
        factor = wide[6:7] * (ratio * jnp.sqrt(ratio))
        powers = [low * exp_z[c : c + 1] for c in range(FZ)]
        powers += [high * jnp.where(upper, exp_z[c : c + 1], exp_z[c + 3 : c + 4]) for c in range(3)]
        return [factor * jnp.maximum(power - floor, 0.0) for power in powers]

    total = charge_of(4)

    group256 = double(group)

    def along_x_forward(values, store):
        count = values.shape[0]
        high, low = split2(values)
        both = jnp.concatenate([high, low], axis=0)
        for p in range(NY // 2):
            rep_h, rep_l = spans(p)
            out = dot(both, rep_h)
            out = out[:count] + (out[count:] + dot(high, rep_l))
            for i in range(count // 72):
                chosen = out[72 * i : 72 * i + 8]
                for g in range(1, 9):
                    chosen = jnp.where(group256 >= g, out[72 * i + 8 * g : 72 * i + 8 * g + 8], chosen)
                store(2 * p, i, chosen[:, :128])
                store(2 * p + 1, i, chosen[:, 128:])

    def history_along_x(first, count, send):
        def store(j, i, value):
            send[j, i] = value

        rows = slice(72 * first, 72 * (first + count))
        along_x_forward(jnp.concatenate([hist_0[rows, :], hist_1[rows, :]], axis=1), store)

    loads[7].wait()
    lane_h = lax.broadcasted_iota(jnp.int32, (HIST, 128), 1)
    for c in range(FZ):
        for pair in range(FY // 2):
            a, b, d = (history[c, :, 384 * pair + 128 * k : 384 * pair + 128 * k + 128] for k in range(3))
            rolled_b = pltpu.roll(b, 64, 1)
            rolled_d = pltpu.roll(d, 64, 1)
            for y, low, high in (
                (2 * pair, a, jnp.where(lane_h < 64, b, 0.0)),
                (2 * pair + 1, jnp.where(lane_h < 64, rolled_b, rolled_d), jnp.where(lane_h < 64, rolled_d, 0.0)),
            ):
                row = 8 * c + y if y < 8 else 48 + 8 * (c % 3) + 4 * (c // 3) + y - 8
                hist_0[pl.ds(row, HIST, stride=72), :] = low
                hist_1[pl.ds(row, HIST, stride=72), :] = high
    loads[6].wait()
    history_along_x(0, EARLY, send_g)

    whole = planes.at[pl.ds(0, 12)]
    pltpu.make_async_copy(whole, whole, halo_recv).wait()
    parts = split3(planes[...].reshape(144, NC))
    weights = table("ix")
    along_x = dot(parts[0], weights) + dot(parts[1], weights) + dot(parts[2], weights)
    parts = split3(along_x)
    weights = table("spread_y")
    smooth = dot(weights, parts[0]) + dot(weights, parts[1]) + dot(weights, parts[2])

    for kind, slots in ((0, (3, 5)), (1, (1, 7)), (2, (0, 2, 6, 8))):
        whole = atoms.at[pl.ds(0, len(slots))]
        pltpu.make_async_copy(whole, whole, atom_recv.at[kind]).wait()
        for k in slots:
            total = [a + b for a, b in zip(total, charge_of(k))]

    inside = lax.broadcasted_iota(jnp.int32, (8, 256), 1) < NF
    blocks = []
    for g in range(9):
        rows = slice(8 * g, 8 * g + 8)
        given = jnp.concatenate([field_0[rows, :], field_1[rows, :]], axis=1)
        value = jnp.where(inside, smooth[rows] + total[g] - given, 0.0)
        blocks.append(value)
        field_0[rows, :] = value[:, :128]
        field_1[rows, :] = value[:, 128:]

    def exchange_y(send, recv, ssem, rsem):
        def act(j):
            pltpu.make_async_remote_copy(
                send.at[j], recv.at[gy], ssem, rsem, device_id=(gz, j), device_id_type=MESH
            ).start()

        each_partner(gy, NY, act)
        recv[gy] = send[gy]
        whole = recv.at[pl.ds(0, NY - 1)]
        return pltpu.make_async_copy(whole, whole, rsem), pltpu.make_async_copy(whole, whole, ssem)

    def exchange_z(send, recv, ssem, rsem):
        mine = pl.ds(pl.multiple_of(gz * 4, 4), 4)

        def act(j):
            pltpu.make_async_remote_copy(
                send.at[pl.ds(pl.multiple_of(j * 4, 4), 4)], recv.at[mine],
                ssem, rsem, device_id=(j, gy), device_id_type=MESH,
            ).start()

        each_partner(gz, NZ, act)
        recv[mine, :] = send[mine, :]
        whole = recv.at[pl.ds(0, 4 * (NZ - 1))]
        return pltpu.make_async_copy(whole, whole, rsem), pltpu.make_async_copy(whole, whole, ssem)

    pl.semaphore_wait(ring_z_ready, 2)
    high, low = split2(jnp.concatenate(blocks, axis=0))
    both = jnp.concatenate([high, low], axis=0)
    chip = gy // 2
    for part in ((4, 3, 5), (2, 6, 1, 7, 0)):
        done = []
        for away in part:
            p = wrap(chip + away, NY // 2)
            rows = [
                all_tables[pl.ds(pl.multiple_of(place[name][0] + 256 * p, 16), 256), :]
                for name in ("rep_h", "rep_l")
            ]
            out = dot(both, rows[0])
            out = out[:72] + (out[72:] + dot(high, rows[1]))
            chosen = out[0:8]
            for g in range(1, 9):
                chosen = jnp.where(group256 >= g, out[8 * g : 8 * g + 8], chosen)
            done.append((away, p, chosen))
        for away, p, chosen in done:
            send1[2 * p] = chosen[:, :128]
            send1[2 * p + 1] = chosen[:, 128:]
        for away, p, _ in done:
            for j in (2 * p, 2 * p + 1) if away else (other_core,):
                pltpu.make_async_remote_copy(
                    send1.at[j], recv1.at[gy], s1, r1, device_id=(gz, j), device_id_type=MESH
                ).start()
    recv1[gy] = send1[gy]
    whole = recv1.at[pl.ds(0, NY - 1)]
    arrived = pltpu.make_async_copy(whole, whole, r1)
    sent1 = pltpu.make_async_copy(whole, whole, s1)
    arrived_g, sent_g = exchange_y(send_g, recv_g, sg, rg)
    pl.semaphore_wait(ring_y_ready, 2)
    for j in ring_x:
        greet(plane_ready, j, gy)
    history_along_x(EARLY, HIST - EARLY, send_h)
    arrived_h, sent_h = exchange_y(send_h, recv_h, sh, rh)

    groups128 = jnp.concatenate([group] * NY, axis=0)
    rows128 = jnp.concatenate([row8] * NY, axis=0)
    from_upper = (groups128 < 3) & (rows128 < 4)
    from_lower = (groups128 >= 3) & (groups128 < 6) & (rows128 >= 4)
    even_rows = rows128 % 2 == 0

    def along_y_forward(packed):
        moved = jnp.where(
            from_upper, pltpu.roll(packed, 128 - 72, 1), jnp.where(from_lower, pltpu.roll(packed, 128 - 36, 1), 0.0)
        )
        out = dot_data((table("fy_h"), table("fy_l")), jnp.concatenate([packed, moved], axis=0))
        high = out[128:]
        return jnp.where(
            groups128 < 6, out[:128], jnp.where(even_rows, pltpu.roll(high, 72, 1), pltpu.roll(high, 36, 1))
        )

    arrived.wait()
    send2[0:128, :] = along_y_forward(recv1[...].reshape(128, 128))
    pl.semaphore_wait(plane_ready, 3)
    arrived, sent2 = exchange_z(send2, recv2, s2, r2)

    def give(out, first, second):
        for pair in range(FY // 2):
            if pair < 4:
                places = ((0, FZ, 2 * pair),)
            else:
                places = ((0, 3, 40 + 2 * pair), (3, 3, 44 + 2 * pair))
            for top, count, row in places:
                low_lanes = lax.broadcasted_iota(jnp.int32, (count, 128), 1) < 64
                a = first[pl.ds(row, count, stride=8), :]
                b = second[pl.ds(row, count, stride=8), :]
                c = pltpu.roll(first[pl.ds(row + 1, count, stride=8), :], 64, 1)
                d = pltpu.roll(second[pl.ds(row + 1, count, stride=8), :], 64, 1)
                tiles = (a, jnp.where(low_lanes, b, c), jnp.where(low_lanes, c, d))
                for k, tile in enumerate(tiles):
                    out[top : top + count, 384 * pair + 128 * k : 384 * pair + 128 * k + 128] = tile

    give(residual_out, field_0, field_1)
    arrived.wait()

    group1 = group[0:1]

    def swapped(pieces, position):
        result = None
        for b in range(6):
            shift = (KX * (b - position)) % 128
            moved = pltpu.roll(pieces[b], shift, 1) if shift else pieces[b]
            result = moved if result is None else jnp.where(group1 >= b, moved, result)
        return result

    packed_rows = [recv2[pl.ds(r, NZ, stride=4), :] for r in range(4)]
    pieces = packed_rows + [
        jnp.where(group1 < 3, pltpu.roll(packed_rows[r], 128 - 72, 1), pltpu.roll(packed_rows[r + 1], 128 - 36, 1))
        for r in (0, 2)
    ]
    stacked = jnp.concatenate([swapped(pieces, a) for a in range(FZ)], axis=0)
    spectrum = dot_data((table("fz_h"), table("fz_l")), (stacked)) * weight[...]
    back = dot_data((table("gz_h"), table("gz_l")), (spectrum))
    pieces = [back[NZ * a : NZ * a + NZ] for a in range(FZ)]
    pieces = [swapped(pieces, b) for b in range(KY)]
    for r in range(4):
        beside = pltpu.roll(pieces[4 + r // 2], 36 if r % 2 else 72, 1)
        send4[pl.ds(r, NZ, stride=4), :] = jnp.where(group1 < 6, pieces[r], beside)
    arrived, sent4 = exchange_z(send4, recv4, s4, r4)

    for first, count, part, here in ((0, EARLY, recv_g, arrived_g), (EARLY, HIST - EARLY, recv_h, arrived_h)):
        here.wait()

        def one_history(i, _, first=first, part=part):
            hist_y[first + i] = along_y_forward(part[:, i].reshape(128, 128))
            return 0

        lax.fori_loop(0, count, one_history, 0, unroll=True)

    arrived.wait()
    terms = [jnp.zeros((8, 128), F32) for _ in range(HIST + 1)]
    for j in range(NY):
        span = slice(8 * j, 8 * j + 8)
        tile = jnp.where(group < 9, recv4[span, :], 0.0)
        for i in range(HIST):
            terms[i] = terms[i] + hist_y[i, span, :] * tile
        terms[HIST] = terms[HIST] + send2[span, :] * tile
    rows = jnp.concatenate(
        [jnp.sum(t, axis=0, keepdims=True) for t in terms] + [jnp.zeros((7, 128), F32)], axis=0
    ) * (1.0 / float(NF) ** 3)
    column = jnp.sum(rows, axis=1, keepdims=True)
    lane_of = lax.broadcasted_iota(jnp.int32, (16, 128), 1)
    row_of = lax.broadcasted_iota(jnp.int32, (16, 128), 0)
    line = jnp.sum(jnp.where(lane_of == row_of, column, 0.0), axis=0, keepdims=True)

    row_b[gz] = line

    def act_b(j):
        pltpu.make_async_remote_copy(
            row_b.at[gz], row_b.at[gz], sb, rb, device_id=(j, gy), device_id_type=MESH
        ).start()

    each_partner(gz, NZ, act_b)

    packed = recv4[0:128, :]
    moved = jnp.where(
        even_rows & (groups128 < 3), pltpu.roll(packed, 128 - 72, 1),
        jnp.where((rows128 % 2 == 1) & (groups128 >= 3) & (groups128 < 6), pltpu.roll(packed, 128 - 36, 1), 0.0),
    )
    out = dot_data((table("gy_h"), table("gy_l")), jnp.concatenate([packed, moved], axis=0))
    low, high = out[:128], out[128:]
    packed = jnp.where(
        groups128 < 6, low, jnp.where(rows128 < 4, pltpu.roll(high, 72, 1), pltpu.roll(high, 36, 1))
    )
    for j in range(NY):
        send5[j] = packed[8 * j : 8 * j + 8]
    arrived, sent5 = exchange_y(send5, recv5, s5, r5)
    whole_b = row_b.at[pl.ds(0, NZ - 1)]
    pltpu.make_async_copy(whole_b, whole_b, rb).wait()
    row_a[gy] = jnp.sum(row_b[...], axis=0)

    def act_a(j):
        pltpu.make_async_remote_copy(
            row_a.at[gy], row_a.at[gy], sa, ra, device_id=(gz, j), device_id_type=MESH
        ).start()

    each_partner(gy, NY, act_a)

    arrived.wait()
    potential = jnp.zeros((72, 256), F32)
    for p in range(NY // 2):
        pair = split2(jnp.concatenate([recv5[2 * p], recv5[2 * p + 1]], axis=1))
        masked = [
            jnp.concatenate([jnp.where(group256 == g, part.astype(F32), 0.0) for g in range(9)], axis=0).astype(BF16)
            for part in pair
        ]
        potential = potential + dot3(masked, spans(p), dot_nt)
    out_0[0:72, :] = potential[:, :128]
    out_1[0:72, :] = potential[:, 128:]
    give(potential_out, out_0, out_1)

    whole = atoms.at[pl.ds(0, 8)]
    pltpu.make_async_copy(whole, whole, atom_send).wait()
    whole = planes.at[pl.ds(0, 12)]
    pltpu.make_async_copy(whole, whole, halo_send).wait()
    for copy in (sent1, sent2, sent_g, sent_h, sent4, sent5):
        copy.wait()
    pltpu.make_async_copy(whole_b, whole_b, sb).wait()
    whole_a = row_a.at[pl.ds(0, NY - 1)]
    pltpu.make_async_copy(whole_a, whole_a, sa).wait()
    pltpu.make_async_copy(whole_a, whole_a, ra).wait()
    sums_out[...] = jnp.sum(row_a[...], axis=0)[0, : HIST + 1]


def write_out(*refs):
    copies = [pltpu.make_async_copy(refs[k], refs[3 + k], refs[6].at[k]) for k in range(3)]
    for copy in copies:
        copy.start()
    for copy in copies:
        copy.wait()


def solution(mesh):
    constants, place = tables()

    def local(coarse, density, history, cell, offset, charge, width):
        coarse = jnp.transpose(coarse, (1, 0, 2))
        history = jnp.transpose(history, (1, 0, 2))
        offset = jnp.transpose(offset, (1, 2, 3, 0))
        inputs = (cell, offset, charge, width, coarse, density, history)
        inputs = (*inputs, jnp.asarray(constants))
        vmem = pl.BlockSpec(memory_space=pltpu.VMEM)
        dma = pltpu.SemaphoreType.DMA
        tile = (NY, 8, 128)
        residual, potential, sums = pl.pallas_call(
            functools.partial(kernel, place),
            out_shape=(
                pltpu.VMEM((FZ, FY * NF), F32),
                pltpu.VMEM((FZ, FY * NF), F32),
                pltpu.VMEM((HIST + 1,), F32),
            ),
            in_specs=[pl.BlockSpec(memory_space=pltpu.HBM)] * len(inputs),
            out_specs=(vmem, vmem, vmem),
            scratch_shapes=[
                *(pltpu.VMEM(i.shape, i.dtype) for i in inputs),
                pltpu.VMEM((18, 8, NC), F32),
                pltpu.VMEM((9, 8, 128), F32),
                *[pltpu.VMEM((128, 128), F32)] * 4,
                *[pltpu.VMEM((648, 128), F32)] * 2,
                *[pltpu.VMEM(tile, F32)] * 2,
                *[pltpu.VMEM((136, 128), F32)] * 4,
                *[pltpu.VMEM(tile, F32)] * 2,
                *[pltpu.VMEM((NY, EARLY, 8, 128), F32)] * 2,
                *[pltpu.VMEM((NY, HIST - EARLY, 8, 128), F32)] * 2,
                pltpu.VMEM((NF, 128), F32),
                pltpu.VMEM((NY, 1, 128), F32),
                pltpu.VMEM((NZ, 1, 128), F32),
                pltpu.VMEM((HIST, 128, 128), F32),
                dma((8,)), dma, dma, dma, dma((3,)),
                *[dma] * 16,
                *[pltpu.SemaphoreType.REGULAR] * 3,
            ],
            compiler_params=pltpu.CompilerParams(collective_id=0, has_side_effects=True),
        )(*inputs)
        results = tuple(pltpu.with_memory_space_constraint(r, pltpu.VMEM) for r in (residual, potential, sums))
        hbm = pl.BlockSpec(memory_space=pltpu.HBM)
        return pl.pallas_call(
            write_out,
            out_shape=tuple(jax.ShapeDtypeStruct(r.shape, F32) for r in results),
            in_specs=[vmem] * 3,
            out_specs=(hbm,) * 3,
            scratch_shapes=[dma((3,))],
        )(*results)

    in_specs = (
        P(None, "gy", None),
        P("gz", "gy"),
        P(None, "gz", "gy"),
        P("gz", "gy", None),
        P(None, "gz", "gy", None),
        P("gz", "gy", None),
        P("gz", "gy", None),
    )
    out_specs = (P("gz", "gy"), P("gz", "gy"), P())
    return jax.shard_map(local, mesh=mesh, in_specs=in_specs, out_specs=out_specs, check_vma=False)
```
